32 devices in a mesh: blk: 8 (over z, y), grp: 4 (over x, core).
Axes of the slice: x: 2, y: 2, z: 4, core: 2. Of those that a mesh axis runs over, the one named last changes fastest.
Arguments:
- frames: bfloat16 [4, 2048, 1024], P('grp', 'blk'), may hold values from -16 to 16
- utt_lengths: int32 [4], replicated, may hold values from 1 to 4096, 8192 in all
- attn_gain: float32 [1024], replicated, may hold values from 0.25 to 1.75
- w_qkv: bfloat16 [1024, 3072], P(None, 'grp'), may hold values from -4 to 4
- w_out: bfloat16 [1024, 1024], replicated, may hold values from -0.375 to 0.375
- conv_gain: float32 [1024], replicated, may hold values from 0.25 to 1.75
- w_glu: bfloat16 [1024, 2048], replicated, may hold values from -0.1875 to 0.1875
- w_depth: float32 [31, 1024], replicated, may hold values from -1 to 1
- depth_gain: float32 [1024], replicated, may hold values from 0.25 to 1.75
- w_proj: bfloat16 [1024, 1024], replicated, may hold values from -0.1875 to 0.1875
Outputs:
- block_out: bfloat16 [4, 2048, 1024], P('grp', 'blk')
The draws below stay inside these ranges and needn't reach their ends.
Inputs may be any that keep to these rules, and one draw needn't show every extreme that they name: `utt_lengths`: they sum to 8192 and the longest is exactly 4096.
All inputs are finite; a program needn't handle non-finite values.
Results may differ from the reference program's by a relative error of at most 0.0095.
Values may be sent and summed in bfloat16 or wider, within the bound.
A program may use at most 192 MiB of HBM per device.

```python
import math
import jax
import jax.numpy as jnp
import numpy as np
from jax import lax

D = 1024
HEADS = 16
KERNEL = 31
WINDOW = 2048
GROUPS = 4
TOKENS = 8192
UTT_MOST = 4096
UTTERANCES = 4


def draw_frames(key, part):
    base_key = jax.random.fold_in(jax.random.fold_in(key, 11), 0)
    drawn = jax.random.normal(base_key, (GROUPS, WINDOW, D), jnp.float32)
    return jnp.clip(drawn, -16.0, 16.0).astype(jnp.bfloat16)


def draw_w_qkv(key, part):
    drawn = jax.random.normal(jax.random.fold_in(key, 23), (D, HEADS, 3, D // HEADS), jnp.float32) * (1.4 / math.sqrt(D))
    return jnp.clip(drawn.reshape(D, 3 * D), -4.0, 4.0).astype(jnp.bfloat16)


def length_profile(amount, total, most, slope):
    loads = [(1 << 20) // math.isqrt(grade ** slope) + 1 for grade in range(2, amount + 1)]
    surplus, counts = total - most - (amount - 1), [1] * (amount - 1)
    while surplus > 0:
        candidates = [i for i in range(amount - 1) if counts[i] < most]
        pool, remaining = sum([loads[i] for i in candidates]), surplus
        for i in candidates:
            addition = min(most - counts[i], max(1, remaining * loads[i] // pool), surplus)
            counts[i] = counts[i] + addition
            surplus = surplus - addition
    return np.array([most] + counts)


def ragged(own_key, count, total, reach, slope):
    if count == 2:
        one = jax.random.randint(own_key, (), max(1, total - reach), min(reach, total - 1) + 1)
        return jnp.stack([one, total - one])
    sizes = jnp.asarray(length_profile(count, total, reach, slope), jnp.int32)
    pairs = (count - 1) // 2
    donor, taker = sizes[1:1 + 2 * pairs:2], sizes[2:2 + 2 * pairs:2]
    slack = jnp.minimum(donor - 1, reach - taker)
    moved = jax.random.randint(jax.random.fold_in(own_key, 1), (pairs,), 0, 1 << 20) % (slack + 1)
    sizes = sizes.at[1:1 + 2 * pairs:2].set(donor - moved).at[2:2 + 2 * pairs:2].set(taker + moved)
    return sizes[jax.random.permutation(jax.random.fold_in(own_key, 2), count)]


def centred(stream_key, shape, scale, limit, held_as=jnp.bfloat16):
    values = scale * jax.random.normal(stream_key, shape, jnp.float32)
    return jnp.clip(values, min=-limit, max=limit).astype(held_as)


def setup_inputs(seed: int = 0) -> dict:
    splits = jax.random.split(jax.random.key(seed), 11)
    return {
        "frames": draw_frames(jax.random.fold_in(splits[10], 71), 0),
        "utt_lengths": ragged(splits[1], UTTERANCES, TOKENS, UTT_MOST, 2).astype(jnp.int32),
        "attn_gain": jnp.clip(1.0 + 0.15 * jax.random.normal(splits[2], (D,), jnp.float32), 0.25, 1.75),
        "w_qkv": draw_w_qkv(jax.random.fold_in(splits[10], 71), 0),
        "w_out": centred(splits[4], (D, D), (D // 4) ** -0.5, 0.375),
        "conv_gain": jnp.clip(1.0 + 0.15 * jax.random.normal(splits[5], (D,), jnp.float32), 0.25, 1.75),
        "w_glu": centred(splits[6], (D, 2 * D), D ** -0.5, 0.1875),
        "w_depth": centred(splits[7], (KERNEL, D), KERNEL ** -0.5, 1.0, jnp.float32),
        "depth_gain": jnp.clip(1.0 + 0.15 * jax.random.normal(splits[8], (D,), jnp.float32), 0.25, 1.75),
        "w_proj": centred(splits[9], (D, D), D ** -0.5, 0.1875),
    }


epsilon = 1e-05
big_negative = -1e+30

def normalize(values, row_gain):
    center = values - lax.optimization_barrier(jnp.mean(values, axis=-1, keepdims=True))
    spread = lax.optimization_barrier(jnp.mean(center * center, axis=-1, keepdims=True))
    return center * lax.rsqrt(spread + epsilon) * row_gain

def segment_of(utt_lengths, positions):
    starts = jnp.cumsum(utt_lengths) - utt_lengths
    started = (starts[None, :] <= positions[:, None]).astype(jnp.int32)
    return lax.optimization_barrier(jnp.sum(started, axis=1)) - 1

def one_head(head_qkv, seg_row, score_scale):
    scores = jnp.dot(head_qkv[0], head_qkv[1].T, preferred_element_type=jnp.float32) * score_scale
    allowed = seg_row[:, None] == seg_row[None, :]
    row_max = lax.optimization_barrier(jnp.max(jnp.where(allowed, scores, big_negative), axis=1, keepdims=True))
    weights = jnp.where(allowed, jnp.exp(scores - row_max), 0.0)
    row_total = lax.optimization_barrier(jnp.sum(weights, axis=1, keepdims=True))
    mixed_values = jnp.dot(weights.astype(jnp.bfloat16), head_qkv[2], preferred_element_type=jnp.float32)
    return mixed_values / row_total

def reference(frames, utt_lengths, attn_gain, w_qkv, w_out, conv_gain, w_glu, w_depth, depth_gain, w_proj):
    head_width = D // HEADS
    kernel_half = (KERNEL - 1) // 2
    score_scale = head_width ** (-0.5)
    flat_frames = frames.reshape(TOKENS, D)
    flat_float = flat_frames.astype(jnp.float32)
    frame_seg = segment_of(utt_lengths, jnp.arange(TOKENS, dtype=jnp.int32))
    normed = normalize(flat_float, attn_gain).astype(jnp.bfloat16)
    qkv_rows = jnp.dot(normed, w_qkv, preferred_element_type=jnp.float32).astype(jnp.bfloat16)
    arranged = jnp.transpose(qkv_rows.reshape(GROUPS, WINDOW, HEADS, 3, head_width), (0, 2, 3, 1, 4))
    group_seg = frame_seg.reshape(GROUPS, WINDOW)

    def one_group(operands):
        group_qkv, seg_row = operands
        return lax.map(lambda head_qkv: one_head(head_qkv, seg_row, score_scale), group_qkv)
    heads_out = lax.map(one_group, (arranged, group_seg))
    attended = jnp.transpose(heads_out, (0, 2, 1, 3)).reshape(TOKENS, D).astype(jnp.bfloat16)
    residual = (flat_float + jnp.dot(attended, w_out, preferred_element_type=jnp.float32)).astype(jnp.bfloat16)
    residual = lax.optimization_barrier(residual)
    conv_in = normalize(residual.astype(jnp.float32), conv_gain).astype(jnp.bfloat16)
    projected = jnp.dot(conv_in, w_glu, preferred_element_type=jnp.float32)
    gated = (projected[:, :D] * jax.nn.sigmoid(projected[:, D:])).astype(jnp.bfloat16)
    gated = lax.optimization_barrier(gated)
    padded = jnp.pad(gated.astype(jnp.float32), ((kernel_half, kernel_half), (0, 0)))
    pad_seg = segment_of(utt_lengths, jnp.arange(-kernel_half, TOKENS + kernel_half, dtype=jnp.int32))
    mixed_conv = jnp.zeros((TOKENS, D), jnp.float32)
    for offset in range(KERNEL):
        same_seg = (pad_seg[offset:offset + TOKENS] == frame_seg)[:, None]
        mixed_conv = mixed_conv + jnp.where(same_seg, padded[offset:offset + TOKENS] * w_depth[offset], 0.0)
    normed_conv = normalize(mixed_conv, depth_gain)
    activated = (normed_conv * jax.nn.sigmoid(normed_conv)).astype(jnp.bfloat16)
    result = (residual.astype(jnp.float32) + jnp.dot(activated, w_proj, preferred_element_type=jnp.float32)).astype(jnp.bfloat16)
    return result.reshape(GROUPS, WINDOW, D)
```

```python
import functools
import math

import jax
import jax.numpy as jnp
from jax import lax
from jax.experimental import pallas as pl
from jax.experimental.pallas import tpu as pltpu
from jax.sharding import PartitionSpec as P

HEADS = 16

epsilon = 1e-05
big_negative = -1e30
MESH = pl.DeviceIdType.MESH
VMEM_LIMIT = 56 * 1024 * 1024


def normalize(values, row_gain):
    center = values - jnp.mean(values, axis=-1, keepdims=True)
    spread = jnp.mean(center * center, axis=-1, keepdims=True)
    return center * lax.rsqrt(spread + epsilon) * row_gain


def starts_of(lengths_ref):
    starts, total = [], jnp.int32(0)
    for c in range(lengths_ref.shape[0]):
        starts.append(total)
        total = total + lengths_ref[c]
    return starts


def seg_at(starts, positions):
    seg = jnp.full(positions.shape, -1, jnp.int32)
    for start in starts:
        seg = seg + jnp.where(positions >= start, 1, 0)
    return seg


def remote(src, dst, send, recv, blk, grp):
    return pltpu.make_async_remote_copy(
        src_ref=src, dst_ref=dst, send_sem=send, recv_sem=recv,
        device_id=(blk, grp), device_id_type=MESH,
    )


def place_of(window, groups):
    return (window % 2) * (groups // 2) + window // 2


def window_at(place, groups):
    return (place % (groups // 2)) * 2 + place // (groups // 2)


def block_kernel(
    blocks, groups, chunks, head_width,
    lengths_ref, frames_ref, gain_ref, conv_gain_ref, depth_ref, depth_gain_ref,
    w_ref, w_out_ref, w_glu_ref, w_proj_ref,
    out_ref,
    norm, held, weights, q_ref, k_ref, v_ref,
    mixed_heads, parts, w_out, w_glu, w_proj, masks, residual, edge, halo, extended, mixed,
    load_sem, d_sem, x_sem, y_sem, p_sem, r_sem, s_sem, a_sem, hs_sem, hr_sem,
):
    b, g = lax.axis_index("blk"), lax.axis_index("grp")
    np_ = blocks // groups
    pairs = groups // 2
    rows, width = norm.shape[1:]
    block = rows * chunks
    columns = weights.shape[1]
    heads = columns // (3 * head_width)
    taps = depth_ref.shape[0]
    half = (taps - 1) // 2
    rim = halo.shape[1]
    place, share, core, chip = b // np_, b % np_, g % 2, g // 2
    mine = window_at(place, groups)
    source_chip = mine // 2
    partner = g + 1 - 2 * core
    unit_index = g * np_ + share
    home = mine == g
    position = g * blocks + b
    if np_ == 1:
        w_src = w_ref
    else:
        w_src = w_ref.at[:, pl.ds(pl.multiple_of(share * columns, 128), columns)]
    loads = [
        pltpu.make_async_copy(w_src, weights, load_sem.at[0]),
        pltpu.make_async_copy(w_out_ref, w_out, load_sem.at[1]),
        pltpu.make_async_copy(w_glu_ref, w_glu, load_sem.at[2]),
        pltpu.make_async_copy(w_proj_ref, w_proj, load_sem.at[3]),
    ]
    loads[0].start()
    target = place_of(g, groups) * np_ + share
    target_core = place % 2
    self_kept = jnp.logical_and(target == b, target_core == core)

    def direct(c):
        u = b * chunks + c
        return remote(
            norm.at[c], held.at[u], d_sem.at[c], r_sem.at[u], target, 2 * chip + target_core
        )

    with jax.named_scope("norm"):
        for c in range(chunks):
            part = frames_ref[c * rows:(c + 1) * rows, :].astype(jnp.float32)
            norm[c] = normalize(part, gain_ref[...]).astype(jnp.bfloat16)

            @pl.when(jnp.logical_not(self_kept))
            def _():
                direct(c).start()

            @pl.when(self_kept)
            def _():
                held[b * chunks + c] = norm[c]

    for load in loads[1:]:
        load.start()

    lane = lax.broadcasted_iota(jnp.int32, (rows, 128), 1)
    row = lax.broadcasted_iota(jnp.int32, (rows, 128), 0)
    scale = head_width ** (-0.5) * math.log2(math.e)
    starts = starts_of(lengths_ref)

    for h in range(heads):
        at_row = lax.broadcasted_iota(jnp.int32, (16, v_ref.shape[2]), 0)
        v_ref[h, head_width:, :] = jnp.where(at_row == 0, 1.0, 0.0).astype(jnp.bfloat16)

    def padded(part):
        return jnp.concatenate([part, jnp.zeros((rows, 128 - head_width), jnp.float32)], axis=1)

    def project(u):
        out = jnp.dot(held[u], weights[...], preferred_element_type=jnp.float32)
        seg = seg_at(starts, mine * blocks * chunks * rows + u * rows + row)
        same = lane - head_width == seg
        at = pl.ds(pl.multiple_of(u * rows, rows), rows)
        for h in range(heads):
            o = 3 * head_width * h
            q = padded(out[:, o:o + head_width] * scale)
            k = padded(out[:, o + head_width:o + 2 * head_width])
            v = out[:, o + 2 * head_width:o + 3 * head_width]
            q = jnp.where(lane < head_width, q, jnp.where(same, big_negative, 0.0))
            k = jnp.where(lane < head_width, k, jnp.where(same, 0.0, 1.0))
            q_ref[h, at, :] = q.astype(jnp.bfloat16)
            k_ref[h, at, :] = k.astype(jnp.bfloat16)
            v_ref[h, :head_width, at] = v.T.astype(jnp.bfloat16)

    def pair(u):
        return remote(held.at[u], held.at[u], p_sem.at[u], r_sem.at[u], b, partner)

    def across(u, i):
        other = b - share + (share + i) % np_
        return remote(held.at[u], held.at[u], y_sem.at[u, i], r_sem.at[u], other, g)

    def over(u, k):
        return remote(held.at[u], held.at[u], x_sem.at[u, k], r_sem.at[u], b, 2 * k + core)

    def unit(j, i):
        n = j // chunks
        n = n + place // pairs * (pairs - 1 - 2 * n)
        return ((2 * n + core) * np_ + (share + i) % np_) * chunks + j % chunks

    count = pairs * chunks

    def take(j, carry):
        u = unit(j, 0)

        @pl.when(jnp.logical_not(jnp.logical_and(u // chunks == b, mine == g)))
        def _():
            pair(u).wait_recv()

        for k in range(pairs):
            @pl.when(jnp.logical_and(chip == source_chip, chip != k))
            def _():
                over(u, k).start()

        for i in range(1, np_):
            across(u, i).start()
        pair(u).start()
        return carry

    with jax.named_scope("take"):
        lax.fori_loop(0, count, take, 0)
    loads[0].wait()

    def own(j, carry):
        project(unit(j, 0))
        return carry

    with jax.named_scope("own"):
        lax.fori_loop(0, count, own, 0)

    def pass_on(j, carry):
        for i in range(1, np_):
            u = unit(j, i)
            pair(u).wait_recv()
            pair(u).start()
            project(u)
        return carry

    if np_ > 1:
        with jax.named_scope("pass_on"):
            lax.fori_loop(0, count, pass_on, 0)

    def rest(j, carry):
        n = j // (np_ * chunks)
        n = n + place // pairs * (pairs - 1 - 2 * n)
        i = j // chunks % np_
        u = ((2 * n + 1 - core) * np_ + (share + i) % np_) * chunks + j % chunks
        pair(u).wait_recv()
        project(u)
        return carry

    with jax.named_scope("rest"):
        lax.fori_loop(0, count * np_, rest, 0)

    def send(s):
        return remote(
            mixed_heads.at[s], parts.at[unit_index], s_sem.at[s], a_sem.at[unit_index], s, mine
        )

    def attend_for(i, carry):
        s = (b + 1 + i) % blocks
        at = pl.ds(pl.multiple_of(s * block, block), block)
        mixed_heads[s] = attend(head_width, q_ref, k_ref, v_ref, at)
        kept = jnp.logical_and(home, s == b)

        @pl.when(jnp.logical_not(kept))
        def _():
            send(s).start()

        @pl.when(kept)
        def _():
            parts[unit_index] = mixed_heads[s]

        return carry

    with jax.named_scope("attend"):
        lax.fori_loop(0, blocks, attend_for, 0)

    row = position * block + lax.broadcasted_iota(jnp.int32, (block, 128), 0)
    low = jnp.zeros((block, 128), jnp.int32)
    high = jnp.full((block, 128), blocks * groups * block, jnp.int32)
    for start in starts:
        low = jnp.where(row >= start, jnp.maximum(low, start), low)
        high = jnp.where(row < start, jnp.minimum(high, start), high)
    for t in range(taps):
        at = row + (t - half)
        masks[t] = jnp.where(jnp.logical_and(at >= low, at < high), 1.0, 0.0)

    with jax.named_scope("parts_wait"):
        for i in range(blocks):
            @pl.when(jnp.logical_not(jnp.logical_and(home, unit_index == i)))
            def _():
                remote(parts.at[i], parts.at[i], s_sem.at[i], a_sem.at[i], b, g).wait_recv()

    with jax.named_scope("mid_mm"):
        attended = jnp.concatenate([parts[i] for i in range(blocks)], axis=1)
        loads[1].wait()
        total = frames_ref[...].astype(jnp.float32) + jnp.dot(
            attended, w_out[...], preferred_element_type=jnp.float32
        )
        residual[...] = total.astype(jnp.bfloat16)
        conv_in = normalize(residual[...].astype(jnp.float32), conv_gain_ref[...]).astype(jnp.bfloat16)
        loads[2].wait()
        step = 256
        for n in range(0, width, step):
            a = jnp.dot(conv_in, w_glu[:, n:n + step], preferred_element_type=jnp.float32)
            gate = jnp.dot(
                conv_in, w_glu[:, width + n:width + n + step], preferred_element_type=jnp.float32
            )
            gated = (a * jax.nn.sigmoid(gate)).astype(jnp.bfloat16)
            edge[0, :, n:n + step] = gated[:rim]
            edge[1, :, n:n + step] = gated[block - rim:]
            for c in range(0, step, 128):
                extended[(n + c) // 128, rim:rim + block, :] = gated[:, c:c + 128].astype(jnp.float32)

    after = (position + 1) % (blocks * groups)
    before = (position + blocks * groups - 1) % (blocks * groups)
    to_next = remote(
        edge.at[1], halo.at[0], hs_sem.at[1], hr_sem.at[0], after % blocks, after // blocks
    )
    to_prev = remote(
        edge.at[0], halo.at[1], hs_sem.at[0], hr_sem.at[1], before % blocks, before // blocks
    )
    to_next.start()
    to_prev.start()

    strip = min(64, block)
    spans = -(-taps // 8)

    def convolve(strips):
        def column(c, carry):
            cols = pl.ds(pl.multiple_of(c * 128, 128), 128)
            for r in strips:
                acc = jnp.zeros((strip, 128), jnp.float32)
                for p in range(8):
                    o = rim + r + p - half
                    slab = extended[c, o:o + strip + 8 * (spans - 1), :]
                    for j in range(spans):
                        t = 8 * j + p
                        if t < taps:
                            x = slab[8 * j:8 * j + strip] * masks[t, r:r + strip, :]
                            acc = acc + x * depth_ref[t:t + 1, cols]
                mixed[r:r + strip, cols] = acc
            return carry

        lax.fori_loop(0, width // 128, column, 0)

    every = list(range(0, block, strip))
    with jax.named_scope("conv_mid"):
        convolve(every[1:-1])
    with jax.named_scope("halo_wait"):
        to_next.wait_recv()
        to_prev.wait_recv()
    with jax.named_scope("conv_edge"):
        for c in range(width // 128):
            extended[c, :rim, :] = halo[0, :, 128 * c:128 * c + 128].astype(jnp.float32)
            extended[c, rim + block:2 * rim + block, :] = halo[1, :, 128 * c:128 * c + 128].astype(jnp.float32)
        convolve([every[0], every[-1]])
    with jax.named_scope("tail_mm"):
        normed = normalize(mixed[...], depth_gain_ref[...])
        activated = (normed * jax.nn.sigmoid(normed)).astype(jnp.bfloat16)
        loads[3].wait()
        out_ref[0] = (
            residual[...].astype(jnp.float32)
            + jnp.dot(activated, w_proj[...], preferred_element_type=jnp.float32)
        ).astype(out_ref.dtype)

    for c in range(chunks):
        @pl.when(jnp.logical_not(self_kept))
        def _():
            direct(c).wait_send()

    def drain(j, carry):
        u = unit(j, 0)
        for k in range(pairs):
            @pl.when(jnp.logical_and(chip == source_chip, chip != k))
            def _():
                over(u, k).wait_send()

        for i in range(1, np_):
            across(u, i).wait_send()
        for i in range(np_):
            pair(unit(j, i)).wait_send()
        return carry

    lax.fori_loop(0, count, drain, 0)

    for i in range(blocks):
        @pl.when(jnp.logical_not(jnp.logical_and(home, b == i)))
        def _():
            send(i).wait_send()

    to_next.wait_send()
    to_prev.wait_send()


def attend(head_width, q_ref, k_ref, v_ref, at):
    outs = []
    for h in range(q_ref.shape[0]):
        scores = lax.dot_general(
            k_ref[h], q_ref[h, at, :], (((1,), (1,)), ((), ())),
            preferred_element_type=jnp.float32,
        )
        top = jnp.max(scores, axis=0, keepdims=True)
        weights = jnp.exp2(scores - top).astype(jnp.bfloat16)
        mixed = jnp.dot(v_ref[h], weights, preferred_element_type=jnp.float32)
        outs.append(mixed[:head_width] / mixed[head_width:head_width + 1])
    return jnp.concatenate(outs, axis=0).T.astype(jnp.bfloat16)


def body(
    frames, utt_lengths, attn_gain, w_qkv, w_out, conv_gain, w_glu, w_depth, depth_gain, w_proj
):
    rows, width = frames.shape[1:]
    blocks, groups = lax.axis_size("blk"), lax.axis_size("grp")
    head_width = width // HEADS
    np_ = blocks // groups
    columns = w_qkv.shape[1] // np_
    heads = columns // (3 * head_width)
    window = rows * blocks
    chunks = 2 if rows % 32 == 0 else 1
    taps = w_depth.shape[0]
    rim = -(-(taps // 2) // 16) * 16
    vm = pl.BlockSpec(memory_space=pltpu.VMEM)
    hbm = pl.BlockSpec(memory_space=pl.ANY)
    return pl.pallas_call(
        functools.partial(block_kernel, blocks, groups, chunks, head_width),
        out_shape=jax.ShapeDtypeStruct((1, rows, width), jnp.bfloat16),
        in_specs=[pl.BlockSpec(memory_space=pltpu.SMEM)] + [vm] * 5 + [hbm] * 4,
        out_specs=vm,
        scratch_shapes=[
            pltpu.VMEM((chunks, rows // chunks, width), jnp.bfloat16),
            pltpu.VMEM((blocks * chunks, rows // chunks, width), jnp.bfloat16),
            pltpu.VMEM((width, columns), jnp.bfloat16),
            pltpu.VMEM((heads, window, 128), jnp.bfloat16),
            pltpu.VMEM((heads, window, 128), jnp.bfloat16),
            pltpu.VMEM((heads, head_width + 16, window), jnp.bfloat16),
            pltpu.VMEM((blocks, rows, heads * head_width), jnp.bfloat16),
            pltpu.VMEM((blocks, rows, heads * head_width), jnp.bfloat16),
            pltpu.VMEM(w_out.shape, jnp.bfloat16),
            pltpu.VMEM(w_glu.shape, jnp.bfloat16),
            pltpu.VMEM(w_proj.shape, jnp.bfloat16),
            pltpu.VMEM((taps, rows, 128), jnp.float32),
            pltpu.VMEM((rows, width), jnp.bfloat16),
            pltpu.VMEM((2, rim, width), jnp.bfloat16),
            pltpu.VMEM((2, rim, width), jnp.bfloat16),
            pltpu.VMEM((width // 128, rows + 2 * rim + 8, 128), jnp.float32),
            pltpu.VMEM((rows, width), jnp.float32),
            pltpu.SemaphoreType.DMA((4,)),
            pltpu.SemaphoreType.DMA((chunks,)),
            pltpu.SemaphoreType.DMA((blocks * chunks, groups // 2)),
            pltpu.SemaphoreType.DMA((blocks * chunks, np_)),
            pltpu.SemaphoreType.DMA((blocks * chunks,)),
            pltpu.SemaphoreType.DMA((blocks * chunks,)),
            pltpu.SemaphoreType.DMA((blocks,)),
            pltpu.SemaphoreType.DMA((blocks,)),
            pltpu.SemaphoreType.DMA((2,)),
            pltpu.SemaphoreType.DMA((2,)),
        ],
        compiler_params=pltpu.CompilerParams(has_side_effects=True, vmem_limit_bytes=VMEM_LIMIT),
        name="block",
    )(
        utt_lengths, frames[0], attn_gain[None], conv_gain[None], w_depth, depth_gain[None],
        w_qkv, w_out, w_glu, w_proj,
    )


def solution(mesh):
    in_specs = (P("grp", "blk", None), P(), P(), P(None, "grp"), P(), P(), P(), P(), P(), P())
    out_specs = P("grp", "blk", None)
    return jax.shard_map(body, mesh=mesh, in_specs=in_specs, out_specs=out_specs, check_vma=False)
```

```python
import functools
import math

import jax
import jax.numpy as jnp
from jax import lax
from jax.experimental import pallas as pl
from jax.experimental.pallas import tpu as pltpu
from jax.sharding import PartitionSpec as P

HEADS = 16

epsilon = 1e-05
big_negative = -1e30
MESH = pl.DeviceIdType.MESH
VMEM_LIMIT = 56 * 1024 * 1024


def normalize(values, row_gain):
    center = values - jnp.mean(values, axis=-1, keepdims=True)
    spread = jnp.mean(center * center, axis=-1, keepdims=True)
    return center * lax.rsqrt(spread + epsilon) * row_gain


def starts_of(lengths_ref):
    starts, total = [], jnp.int32(0)
    for c in range(lengths_ref.shape[0]):
        starts.append(total)
        total = total + lengths_ref[c]
    return starts


def seg_at(starts, positions):
    seg = jnp.full(positions.shape, -1, jnp.int32)
    for start in starts:
        seg = seg + jnp.where(positions >= start, 1, 0)
    return seg


def remote(src, dst, send, recv, blk, grp):
    return pltpu.make_async_remote_copy(
        src_ref=src, dst_ref=dst, send_sem=send, recv_sem=recv,
        device_id=(blk, grp), device_id_type=MESH,
    )


def slot_of(b, g, blocks):
    half = blocks // 2
    return (b % half + (g % 2 + g // 2) * half) % blocks


def block_kernel(
    blocks, groups, parts_of_chunk, head_width,
    lengths_ref, frames_in, gain_in, conv_gain_in, depth_in, depth_gain_in,
    w_ref, w_out_ref, w_glu_ref, w_proj_ref,
    out_ref,
    frames_ref, gain_ref, conv_gain_ref, depth_ref, depth_gain_ref, norm, held, weights, lent, q_ref, k_ref, v_ref, scores,
    mixed_heads, parts, w_out, w_glu, w_proj, masks, residual, edge, halo, extended, mixed,
    load_sem, in_sem, ws_sem, wr_sem, d_sem, x_sem, y_sem, p_sem, r_sem, s_sem, a_sem, hs_sem, hr_sem,
):
    b, g = lax.axis_index("blk"), lax.axis_index("grp")
    np_ = blocks // groups
    steps = blocks // np_
    reach = steps // 2
    rows, width = held.shape[1:]
    chunks = norm.shape[0]
    block = rows * chunks
    part_rows = rows // parts_of_chunk
    columns = weights.shape[1]
    heads = columns // (3 * head_width)
    taps = depth_ref.shape[0]
    half = (taps - 1) // 2
    rim = halo.shape[1]
    step, share, core, chip = b // np_, b % np_, g % 2, g // 2
    side = step // reach
    mine = 2 * chip + side
    partner = g + 1 - 2 * core
    slot = slot_of(b, g, blocks)
    home = mine == g
    position = g * blocks + b

    after = (position + 1) % (blocks * groups)
    before = (position + blocks * groups - 1) % (blocks * groups)
    barrier = pltpu.get_barrier_semaphore()

    def hail(other_b, other_g):
        pl.semaphore_signal(
            barrier, inc=1, device_id=(other_b, other_g), device_id_type=MESH
        )

    for c in range(2):
        def hail_row(i, carry):
            @pl.when(jnp.logical_or(i != b, core != c))
            def _():
                hail(i, 2 * chip + c)

            return carry

        lax.fori_loop(0, blocks, hail_row, 0)
    for other in range(groups):
        @pl.when(chip != other // 2)
        def _():
            hail(b, other)

    callers = 2 * blocks - 1 + groups - 2
    for near in (after, before):
        apart = near // blocks // 2 != chip

        @pl.when(apart)
        def _():
            hail(near % blocks, near // blocks)

        callers = callers + jnp.where(apart, 1, 0)

    inputs = [
        pltpu.make_async_copy(src, dst, in_sem.at[i]) for i, (src, dst) in enumerate([
            (frames_in, frames_ref), (gain_in, gain_ref), (conv_gain_in, conv_gain_ref),
            (depth_in, depth_ref), (depth_gain_in, depth_gain_ref),
        ])
    ]
    for copy in inputs:
        copy.start()

    def slab_of(sub):
        if np_ == 1:
            return w_ref
        return w_ref.at[:, pl.ds(pl.multiple_of(sub * columns, 128), columns)]

    own_slab = slot // np_ == g
    load_own = pltpu.make_async_copy(slab_of(b % np_), weights, load_sem.at[0])
    load_lent = pltpu.make_async_copy(slab_of(b % np_), lent, load_sem.at[4])

    def give(other):
        return slot_of(b, other, blocks) // np_, remote(
            lent, weights, ws_sem.at[other], wr_sem.at[0], b, other
        )

    @pl.when(own_slab)
    def _():
        load_own.start()

    load_lent.start()

    loads = [
        pltpu.make_async_copy(w_out_ref, w_out, load_sem.at[1]),
        pltpu.make_async_copy(w_glu_ref, w_glu, load_sem.at[2]),
        pltpu.make_async_copy(w_proj_ref, w_proj, load_sem.at[3]),
    ]

    def entry(n, at_side):
        first = at_side * reach
        return jnp.clip(n, first, first + reach - 1)

    target = entry(step, core) * np_ + share
    target_core = step % 2
    self_kept = jnp.logical_and(target == b, target_core == core)

    def piece(ref, u, k):
        return ref.at[u, pl.ds(k * part_rows, part_rows)]

    def direct(c, k):
        u = b * chunks + c
        return remote(
            piece(norm, c, k), piece(held, u, k), d_sem.at[c * parts_of_chunk + k], r_sem.at[u * parts_of_chunk + k],
            target, 2 * chip + target_core,
        )

    with jax.named_scope("in_wait"):
        for copy in inputs:
            copy.wait()
    with jax.named_scope("norm"):
        for c in range(chunks):
            part = frames_ref[c * rows:(c + 1) * rows, :].astype(jnp.float32)
            norm[c] = normalize(part, gain_ref[...]).astype(jnp.bfloat16)
    with jax.named_scope("barrier"):
        pl.semaphore_wait(barrier, callers)
    for c in range(chunks):
        for k in range(parts_of_chunk):
            at = slice(k * part_rows, (k + 1) * part_rows)

            @pl.when(jnp.logical_not(self_kept))
            def _():
                direct(c, k).start()

            @pl.when(self_kept)
            def _():
                held[b * chunks + c, at] = norm[c, at]

    load_lent.wait()
    for other in range(groups):
        source, copy = give(other)

        @pl.when(jnp.logical_and(source == g, other != g))
        def _():
            copy.start()

    for load in loads:
        load.start()

    lane = lax.broadcasted_iota(jnp.int32, (rows, 128), 1)
    row = lax.broadcasted_iota(jnp.int32, (rows, 128), 0)
    scale = head_width ** (-0.5) * math.log2(math.e)
    starts = starts_of(lengths_ref)

    for h in range(heads):
        at_row = lax.broadcasted_iota(jnp.int32, (16, v_ref.shape[2]), 0)
        v_ref[h, head_width:, :] = jnp.where(at_row == 0, 1.0, 0.0).astype(jnp.bfloat16)

    def padded(part):
        return jnp.concatenate([part, jnp.zeros((rows, 128 - head_width), jnp.float32)], axis=1)

    def project(u):
        out = jnp.dot(held[u], weights[...], preferred_element_type=jnp.float32)
        seg = seg_at(starts, mine * blocks * chunks * rows + u * rows + row)
        same = lane - head_width == seg
        at = pl.ds(pl.multiple_of(u * rows, rows), rows)
        for h in range(heads):
            o = 3 * head_width * h
            q = padded(out[:, o:o + head_width] * scale)
            k = padded(out[:, o + head_width:o + 2 * head_width])
            v = out[:, o + 2 * head_width:o + 3 * head_width]
            q = jnp.where(lane < head_width, q, jnp.where(same, big_negative, 0.0))
            k = jnp.where(lane < head_width, k, jnp.where(same, 0.0, 1.0))
            q_ref[h, at, :] = q.astype(jnp.bfloat16)
            k_ref[h, at, :] = k.astype(jnp.bfloat16)
            v_ref[h, :head_width, at] = v.T.astype(jnp.bfloat16)

    def pair(u, k):
        return remote(
            piece(held, u, k), piece(held, u, k), p_sem.at[u * parts_of_chunk + k], r_sem.at[u * parts_of_chunk + k], b, partner
        )

    def across(u, i, k):
        other = b - share + (share + i) % np_
        return remote(
            piece(held, u, k), piece(held, u, k), y_sem.at[(u * np_ + i) * parts_of_chunk + k], r_sem.at[u * parts_of_chunk + k], other, g
        )

    def over(u, i, k):
        other = side * reach + i
        return remote(
            piece(held, u, k), piece(held, u, k), x_sem.at[(u * reach + i) * parts_of_chunk + k], r_sem.at[u * parts_of_chunk + k],
            other * np_ + share, g,
        )

    def unit(j, i, parity):
        n = j // chunks
        n = n + side * (reach - 1 - 2 * n)
        return ((2 * n + parity) * np_ + (share + i) % np_) * chunks + j % chunks

    count = reach * chunks

    def enters(u):
        return entry(u // (chunks * np_), side) == step

    def take(j):
        u = unit(j, 0, core)
        for k in range(parts_of_chunk):
            @pl.when(jnp.logical_not(jnp.logical_and(u // chunks == b, home)))
            def _():
                pair(u, k).wait_recv()

            for i in range(reach):
                @pl.when(enters(u) & (step != side * reach + i))
                def _():
                    over(u, i, k).start()

            for i in range(1, np_):
                across(u, i, k).start()
            pair(u, k).start()

    def arrive(u):
        for k in range(parts_of_chunk):
            pair(u, k).wait_recv()

    def pass_on(j):
        for i in range(1, np_):
            u = unit(j, i, core)
            for k in range(parts_of_chunk):
                pair(u, k).wait_recv()
                pair(u, k).start()

    with jax.named_scope("first"):
        take(0)
        take(1)
        pass_on(0)

    with jax.named_scope("weights"):
        @pl.when(own_slab)
        def _():
            load_own.wait()

        @pl.when(jnp.logical_not(own_slab))
        def _():
            give(0)[1].wait_recv()

    def gather(j, carry):
        project(unit(j, 0, core))
        u = unit(j, 0, 1 - core)
        arrive(u)
        project(u)

        @pl.when(j + 2 < count)
        def _():
            take(j + 2)

        for i in range(1, np_):
            project(unit(j, i, core))

        @pl.when(j + 1 < count)
        def _():
            pass_on(j + 1)

        for i in range(1, np_):
            u = unit(j, i, 1 - core)
            arrive(u)
            project(u)
        return carry

    with jax.named_scope("gather"):
        lax.fori_loop(0, count, gather, 0)

    def send(s):
        return remote(
            mixed_heads.at[s], parts.at[slot], s_sem.at[s], a_sem.at[slot], s, mine
        )

    tile = min(512, blocks * block)
    tiles = blocks * block // tile

    def order(i):
        return (b + 1 + i) % blocks

    def score(i, h, n, top):
        at = pl.ds(pl.multiple_of(order(i) * block, block), block)
        keys = slice(n * tile, (n + 1) * tile)
        raw = lax.dot_general(
            k_ref[h, keys, :], q_ref[h, at, :], (((1,), (1,)), ((), ())),
            preferred_element_type=jnp.float32,
        )
        scores[h, keys, :] = raw
        return jnp.maximum(top, jnp.max(raw.reshape(tile // 8, 8, block), axis=0))

    def mix(h, n, top, total):
        keys = slice(n * tile, (n + 1) * tile)
        probs = jnp.exp2(scores[h, keys, :] - top).astype(jnp.bfloat16)
        return total + jnp.dot(v_ref[h, :, keys], probs, preferred_element_type=jnp.float32)

    lowest = jnp.full((8, block), -jnp.inf, jnp.float32)

    def attend_for(i, top):
        outs = []
        for h in range(heads):
            top = jnp.max(top, axis=0, keepdims=True)
            later = lowest
            total = jnp.zeros((v_ref.shape[1], block), jnp.float32)
            next_i, next_h = (i, h + 1) if h + 1 < heads else (jnp.minimum(i + 1, blocks - 1), 0)
            if heads == 1:
                for n in range(tiles):
                    total = mix(h, n, top, total)
                for n in range(tiles):
                    later = score(next_i, next_h, n, later)
            else:
                for n in range(tiles):
                    later = score(next_i, next_h, n, later)
                    total = mix(h, n, top, total)
            outs.append(total[:head_width] / total[head_width:head_width + 1])
            top = later
        s = order(i)
        mixed_heads[s] = jnp.concatenate(outs, axis=0).T.astype(jnp.bfloat16)
        kept = jnp.logical_and(home, s == b)

        @pl.when(jnp.logical_not(kept))
        def _():
            send(s).start()

        @pl.when(kept)
        def _():
            parts[slot] = mixed_heads[s]

        return top

    with jax.named_scope("attend"):
        top = lowest
        for n in range(tiles):
            top = score(0, 0, n, top)
        lax.fori_loop(0, blocks, attend_for, top)

    row = position * block + lax.broadcasted_iota(jnp.int32, (block, 128), 0)
    low = jnp.zeros((block, 128), jnp.int32)
    high = jnp.full((block, 128), blocks * groups * block, jnp.int32)
    for start in starts:
        low = jnp.where(row >= start, jnp.maximum(low, start), low)
        high = jnp.where(row < start, jnp.minimum(high, start), high)
    for t in range(taps):
        at = row + (t - half)
        masks[t] = jnp.where(jnp.logical_and(at >= low, at < high), 1.0, 0.0)

    with jax.named_scope("parts_wait"):
        for i in range(blocks):
            @pl.when(jnp.logical_not(jnp.logical_and(home, slot == i)))
            def _():
                remote(parts.at[i], parts.at[i], s_sem.at[i], a_sem.at[i], b, g).wait_recv()

    with jax.named_scope("mid_mm"):
        attended = jnp.concatenate([parts[i] for i in range(blocks)], axis=1)
        loads[0].wait()
        total = frames_ref[...].astype(jnp.float32) + jnp.dot(
            attended, w_out[...], preferred_element_type=jnp.float32
        )
        residual[...] = total.astype(jnp.bfloat16)
        conv_in = normalize(residual[...].astype(jnp.float32), conv_gain_ref[...]).astype(jnp.bfloat16)
        loads[1].wait()
        span = 256
        for n in range(0, width, span):
            a = jnp.dot(conv_in, w_glu[:, n:n + span], preferred_element_type=jnp.float32)
            gate = jnp.dot(
                conv_in, w_glu[:, width + n:width + n + span], preferred_element_type=jnp.float32
            )
            gated = (a * jax.nn.sigmoid(gate)).astype(jnp.bfloat16)
            edge[0, :, n:n + span] = gated[:rim]
            edge[1, :, n:n + span] = gated[block - rim:]
            for c in range(0, span, 128):
                extended[(n + c) // 128, rim:rim + block, :] = gated[:, c:c + 128].astype(jnp.float32)

    to_next = remote(
        edge.at[1], halo.at[0], hs_sem.at[1], hr_sem.at[0], after % blocks, after // blocks
    )
    to_prev = remote(
        edge.at[0], halo.at[1], hs_sem.at[0], hr_sem.at[1], before % blocks, before // blocks
    )
    to_next.start()
    to_prev.start()

    strip = min(64, block)
    spans = -(-taps // 8)

    def convolve(strips):
        def column(c, carry):
            cols = pl.ds(pl.multiple_of(c * 128, 128), 128)
            for r in strips:
                acc = jnp.zeros((strip, 128), jnp.float32)
                for p in range(8):
                    o = rim + r + p - half
                    slab = extended[c, o:o + strip + 8 * (spans - 1), :]
                    for j in range(spans):
                        t = 8 * j + p
                        if t < taps:
                            x = slab[8 * j:8 * j + strip] * masks[t, r:r + strip, :]
                            acc = acc + x * depth_ref[t:t + 1, cols]
                mixed[r:r + strip, cols] = acc
            return carry

        lax.fori_loop(0, width // 128, column, 0)

    every = list(range(0, block, strip))
    with jax.named_scope("conv_mid"):
        convolve(every[1:-1])
    with jax.named_scope("halo_wait"):
        to_next.wait_recv()
        to_prev.wait_recv()
    with jax.named_scope("conv_edge"):
        for c in range(width // 128):
            extended[c, :rim, :] = halo[0, :, 128 * c:128 * c + 128].astype(jnp.float32)
            extended[c, rim + block:2 * rim + block, :] = halo[1, :, 128 * c:128 * c + 128].astype(jnp.float32)
        convolve([every[0], every[-1]])
    with jax.named_scope("tail_mm"):
        normed = normalize(mixed[...], depth_gain_ref[...])
        activated = (normed * jax.nn.sigmoid(normed)).astype(jnp.bfloat16)
        loads[2].wait()
        out_ref[0] = (
            residual[...].astype(jnp.float32)
            + jnp.dot(activated, w_proj[...], preferred_element_type=jnp.float32)
        ).astype(out_ref.dtype)

    with jax.named_scope("drain"):
        for c in range(chunks):
            for k in range(parts_of_chunk):
                @pl.when(jnp.logical_not(self_kept))
                def _():
                    direct(c, k).wait_send()

        for other in range(groups):
            source, copy = give(other)

            @pl.when(jnp.logical_and(source == g, other != g))
            def _():
                copy.wait_send()

        def drain(j, carry):
            u = unit(j, 0, core)
            for k in range(parts_of_chunk):
                for i in range(reach):
                    @pl.when(enters(u) & (step != side * reach + i))
                    def _():
                        over(u, i, k).wait_send()

                for i in range(1, np_):
                    across(u, i, k).wait_send()
                for i in range(np_):
                    pair(unit(j, i, core), k).wait_send()
            return carry

        lax.fori_loop(0, count, drain, 0)

        for i in range(blocks):
            @pl.when(jnp.logical_not(jnp.logical_and(home, b == i)))
            def _():
                send(i).wait_send()

        to_next.wait_send()
        to_prev.wait_send()


def body(
    frames, utt_lengths, attn_gain, w_qkv, w_out, conv_gain, w_glu, w_depth, depth_gain, w_proj
):
    rows, width = frames.shape[1:]
    blocks, groups = lax.axis_size("blk"), lax.axis_size("grp")
    head_width = width // HEADS
    np_ = blocks // groups
    columns = w_qkv.shape[1] // np_
    heads = columns // (3 * head_width)
    window = rows * blocks
    chunks = 2 if rows % 32 == 0 else 1
    parts_of_chunk = 2 if rows // chunks % 32 == 0 else 1
    reach = blocks // np_ // 2
    taps = w_depth.shape[0]
    rim = -(-(taps // 2) // 16) * 16
    vm = pl.BlockSpec(memory_space=pltpu.VMEM)
    hbm = pl.BlockSpec(memory_space=pl.ANY)
    return pl.pallas_call(
        functools.partial(block_kernel, blocks, groups, parts_of_chunk, head_width),
        out_shape=jax.ShapeDtypeStruct((1, rows, width), jnp.bfloat16),
        in_specs=[pl.BlockSpec(memory_space=pltpu.SMEM)] + [hbm] * 9,
        out_specs=vm,
        scratch_shapes=[
            pltpu.VMEM((rows, width), jnp.bfloat16),
            pltpu.VMEM((1, width), jnp.float32),
            pltpu.VMEM((1, width), jnp.float32),
            pltpu.VMEM(w_depth.shape, jnp.float32),
            pltpu.VMEM((1, width), jnp.float32),
            pltpu.VMEM((chunks, rows // chunks, width), jnp.bfloat16),
            pltpu.VMEM((blocks * chunks, rows // chunks, width), jnp.bfloat16),
            pltpu.VMEM((width, columns), jnp.bfloat16),
            pltpu.VMEM((width, columns), jnp.bfloat16),
            pltpu.VMEM((heads, window, 128), jnp.bfloat16),
            pltpu.VMEM((heads, window, 128), jnp.bfloat16),
            pltpu.VMEM((heads, head_width + 16, window), jnp.bfloat16),
            pltpu.VMEM((heads, window, rows), jnp.float32),
            pltpu.VMEM((blocks, rows, heads * head_width), jnp.bfloat16),
            pltpu.VMEM((blocks, rows, heads * head_width), jnp.bfloat16),
            pltpu.VMEM(w_out.shape, jnp.bfloat16),
            pltpu.VMEM(w_glu.shape, jnp.bfloat16),
            pltpu.VMEM(w_proj.shape, jnp.bfloat16),
            pltpu.VMEM((taps, rows, 128), jnp.float32),
            pltpu.VMEM((rows, width), jnp.bfloat16),
            pltpu.VMEM((2, rim, width), jnp.bfloat16),
            pltpu.VMEM((2, rim, width), jnp.bfloat16),
            pltpu.VMEM((width // 128, rows + 2 * rim + 8, 128), jnp.float32),
            pltpu.VMEM((rows, width), jnp.float32),
            pltpu.SemaphoreType.DMA((5,)),
            pltpu.SemaphoreType.DMA((5,)),
            pltpu.SemaphoreType.DMA((groups,)),
            pltpu.SemaphoreType.DMA((1,)),
            pltpu.SemaphoreType.DMA((chunks * parts_of_chunk,)),
            pltpu.SemaphoreType.DMA((blocks * chunks * reach * parts_of_chunk,)),
            pltpu.SemaphoreType.DMA((blocks * chunks * np_ * parts_of_chunk,)),
            pltpu.SemaphoreType.DMA((blocks * chunks * parts_of_chunk,)),
            pltpu.SemaphoreType.DMA((blocks * chunks * parts_of_chunk,)),
            pltpu.SemaphoreType.DMA((blocks,)),
            pltpu.SemaphoreType.DMA((blocks,)),
            pltpu.SemaphoreType.DMA((2,)),
            pltpu.SemaphoreType.DMA((2,)),
        ],
        compiler_params=pltpu.CompilerParams(
            collective_id=0, has_side_effects=True, vmem_limit_bytes=VMEM_LIMIT),
        name="block",
    )(
        utt_lengths, frames[0], attn_gain[None], conv_gain[None], w_depth, depth_gain[None],
        w_qkv, w_out, w_glu, w_proj,
    )


def solution(mesh):
    in_specs = (P("grp", "blk", None), P(), P(), P(None, "grp"), P(), P(), P(), P(), P(), P())
    out_specs = P("grp", "blk", None)
    return jax.shard_map(body, mesh=mesh, in_specs=in_specs, out_specs=out_specs, check_vma=False)
```

```python
import functools
import math

import jax
import jax.numpy as jnp
from jax import lax
from jax.experimental import pallas as pl
from jax.experimental.pallas import tpu as pltpu
from jax.sharding import PartitionSpec as P

HEADS = 16

epsilon = 1e-05
big_negative = -1e30
MESH = pl.DeviceIdType.MESH
VMEM_LIMIT = 56 * 1024 * 1024


def normalize(values, row_gain):
    center = values - jnp.mean(values, axis=-1, keepdims=True)
    spread = jnp.mean(center * center, axis=-1, keepdims=True)
    return center * lax.rsqrt(spread + epsilon) * row_gain


def starts_of(lengths_ref):
    starts, total = [], jnp.int32(0)
    for c in range(lengths_ref.shape[0]):
        starts.append(total)
        total = total + lengths_ref[c]
    return starts


def seg_at(starts, positions):
    seg = jnp.full(positions.shape, -1, jnp.int32)
    for start in starts:
        seg = seg + jnp.where(positions >= start, 1, 0)
    return seg


def remote(src, dst, send, recv, blk, grp):
    return pltpu.make_async_remote_copy(
        src_ref=src, dst_ref=dst, send_sem=send, recv_sem=recv,
        device_id=(blk, grp), device_id_type=MESH,
    )


def slot_of(b, g, blocks):
    half = blocks // 2
    return (b % half + (g % 2 + g // 2) * half) % blocks


def block_kernel(
    blocks, groups, parts_of_chunk, head_width,
    lengths_ref, frames_in, gain_in, conv_gain_in, depth_in, depth_gain_in,
    w_ref, w_out_ref, w_glu_ref, w_proj_ref,
    out_ref,
    frames_ref, gain_ref, conv_gain_ref, depth_ref, depth_gain_ref, norm, held, weights, lent, q_ref, k_ref, v_ref, scores,
    mixed_heads, parts, w_out, w_glu, w_proj, masks, residual, edge, halo, extended, mixed,
    load_sem, in_sem, ws_sem, wr_sem, d_sem, x_sem, y_sem, p_sem, r_sem, s_sem, a_sem, hs_sem, hr_sem,
):
    b, g = lax.axis_index("blk"), lax.axis_index("grp")
    np_ = blocks // groups
    steps = blocks // np_
    reach = steps // 2
    rows, width = held.shape[1:]
    chunks = norm.shape[0]
    block = rows * chunks
    part_rows = rows // parts_of_chunk
    columns = weights.shape[1]
    heads = columns // (3 * head_width)
    taps = depth_ref.shape[0]
    half = (taps - 1) // 2
    rim = halo.shape[1]
    step, share, core, chip = b // np_, b % np_, g % 2, g // 2
    side = step // reach
    mine = 2 * chip + side
    partner = g + 1 - 2 * core
    slot = slot_of(b, g, blocks)
    home = mine == g
    position = g * blocks + b

    after = (position + 1) % (blocks * groups)
    before = (position + blocks * groups - 1) % (blocks * groups)
    barrier = pltpu.get_barrier_semaphore()

    def hail(other_b, other_g):
        pl.semaphore_signal(
            barrier, inc=1, device_id=(other_b, other_g), device_id_type=MESH
        )

    for c in range(2):
        def hail_row(i, carry):
            @pl.when(jnp.logical_or(i != b, core != c))
            def _():
                hail(i, 2 * chip + c)

            return carry

        lax.fori_loop(0, blocks, hail_row, 0)
    for other in range(groups):
        @pl.when(chip != other // 2)
        def _():
            hail(b, other)

    callers = 2 * blocks - 1 + groups - 2
    for near in (after, before):
        apart = near // blocks // 2 != chip

        @pl.when(apart)
        def _():
            hail(near % blocks, near // blocks)

        callers = callers + jnp.where(apart, 1, 0)

    inputs = [
        pltpu.make_async_copy(src, dst, in_sem.at[i]) for i, (src, dst) in enumerate([
            (frames_in, frames_ref), (gain_in, gain_ref), (conv_gain_in, conv_gain_ref),
            (depth_in, depth_ref), (depth_gain_in, depth_gain_ref),
        ])
    ]
    for copy in inputs:
        copy.start()

    def slab_of(sub):
        if np_ == 1:
            return w_ref
        return w_ref.at[:, pl.ds(pl.multiple_of(sub * columns, 128), columns)]

    own_slab = slot // np_ == g
    load_own = pltpu.make_async_copy(slab_of(b % np_), weights, load_sem.at[0])
    load_lent = pltpu.make_async_copy(slab_of(b % np_), lent, load_sem.at[4])

    def give(other):
        return slot_of(b, other, blocks) // np_, remote(
            lent, weights, ws_sem.at[other], wr_sem.at[0], b, other
        )

    @pl.when(own_slab)
    def _():
        load_own.start()

    load_lent.start()

    loads = [
        pltpu.make_async_copy(w_out_ref, w_out, load_sem.at[1]),
        pltpu.make_async_copy(w_glu_ref, w_glu, load_sem.at[2]),
        pltpu.make_async_copy(w_proj_ref, w_proj, load_sem.at[3]),
    ]

    def entry(n, at_side):
        first = at_side * reach
        return jnp.clip(n, first, first + reach - 1)

    target = entry(step, core) * np_ + share
    target_core = step % 2
    self_kept = jnp.logical_and(target == b, target_core == core)

    def piece(ref, u, k):
        return ref.at[u, pl.ds(k * part_rows, part_rows)]

    def direct(c, k):
        u = b * chunks + c
        return remote(
            piece(norm, c, k), piece(held, u, k), d_sem.at[c * parts_of_chunk + k], r_sem.at[u * parts_of_chunk + k],
            target, 2 * chip + target_core,
        )

    with jax.named_scope("in_wait"):
        for copy in inputs:
            copy.wait()
    with jax.named_scope("norm"):
        for c in range(chunks):
            part = frames_ref[c * rows:(c + 1) * rows, :].astype(jnp.float32)
            norm[c] = normalize(part, gain_ref[...]).astype(jnp.bfloat16)
    with jax.named_scope("barrier"):
        pl.semaphore_wait(barrier, callers)
    for c in range(chunks):
        for k in range(parts_of_chunk):
            at = slice(k * part_rows, (k + 1) * part_rows)

            @pl.when(jnp.logical_not(self_kept))
            def _():
                direct(c, k).start()

            @pl.when(self_kept)
            def _():
                held[b * chunks + c, at] = norm[c, at]

    load_lent.wait()
    for other in range(groups):
        source, copy = give(other)

        @pl.when(jnp.logical_and(source == g, other != g))
        def _():
            copy.start()

    for load in loads:
        load.start()

    lane = lax.broadcasted_iota(jnp.int32, (rows, 128), 1)
    row = lax.broadcasted_iota(jnp.int32, (rows, 128), 0)
    scale = head_width ** (-0.5) * math.log2(math.e)
    starts = starts_of(lengths_ref)

    for h in range(heads):
        at_row = lax.broadcasted_iota(jnp.int32, (16, v_ref.shape[2]), 0)
        v_ref[h, head_width:, :] = jnp.where(at_row == 0, 1.0, 0.0).astype(jnp.bfloat16)

    def padded(part):
        return jnp.concatenate([part, jnp.zeros((rows, 128 - head_width), jnp.float32)], axis=1)

    def project(u):
        out = jnp.dot(held[u], weights[...], preferred_element_type=jnp.float32)
        seg = seg_at(starts, mine * blocks * chunks * rows + u * rows + row)
        same = lane - head_width == seg
        at = pl.ds(pl.multiple_of(u * rows, rows), rows)
        for h in range(heads):
            o = 3 * head_width * h
            q = padded(out[:, o:o + head_width] * scale)
            k = padded(out[:, o + head_width:o + 2 * head_width])
            v = out[:, o + 2 * head_width:o + 3 * head_width]
            q = jnp.where(lane < head_width, q, jnp.where(same, big_negative, 0.0))
            k = jnp.where(lane < head_width, k, jnp.where(same, 0.0, 1.0))
            q_ref[h, at, :] = q.astype(jnp.bfloat16)
            k_ref[h, at, :] = k.astype(jnp.bfloat16)
            v_ref[h, :head_width, at] = v.T.astype(jnp.bfloat16)

    def unit(j, i, parity):
        n = j // chunks
        n = n + side * (reach - 1 - 2 * n)
        return ((2 * n + parity) * np_ + (share + i) % np_) * chunks + j % chunks

    def came(u, k):
        here = piece(held, u, k)
        return remote(here, here, p_sem.at[0], r_sem.at[u * parts_of_chunk + k], b, partner)

    def pair(j, i, k):
        u = unit(j, i, core)
        here = piece(held, u, k)
        return remote(
            here, here, p_sem.at[(j * np_ + i) * parts_of_chunk + k],
            r_sem.at[u * parts_of_chunk + k], b, partner,
        )

    def across(j, i, k):
        u = unit(j, 0, core)
        here = piece(held, u, k)
        return remote(
            here, here, y_sem.at[(j * np_ + i - 1) * parts_of_chunk + k],
            r_sem.at[u * parts_of_chunk + k], b - share + (share + i) % np_, g,
        )

    def over(j, i, k):
        u = unit(j, 0, core)
        here = piece(held, u, k)
        other = side * reach + (step - side * reach + i) % reach
        return remote(
            here, here, x_sem.at[(j * (reach - 1) + i - 1) * parts_of_chunk + k],
            r_sem.at[u * parts_of_chunk + k], other * np_ + share, g,
        )

    count = reach * chunks

    def enters(j):
        return entry(unit(j, 0, core) // (chunks * np_), side) == step

    def take(j):
        u = unit(j, 0, core)
        for k in range(parts_of_chunk):
            @pl.when(jnp.logical_not(jnp.logical_and(u // chunks == b, home)))
            def _():
                came(u, k).wait_recv()

            @pl.when(enters(j))
            def _():
                for i in range(1, reach):
                    over(j, i, k).start()

            for i in range(1, np_):
                across(j, i, k).start()
            pair(j, 0, k).start()

    def arrive(u):
        for k in range(parts_of_chunk):
            came(u, k).wait_recv()

    def pass_on(j):
        for i in range(1, np_):
            for k in range(parts_of_chunk):
                came(unit(j, i, core), k).wait_recv()
                pair(j, i, k).start()

    with jax.named_scope("first"):
        take(0)
        take(1)
        pass_on(0)
        if count > 2:
            take(2)

    with jax.named_scope("weights"):
        @pl.when(own_slab)
        def _():
            load_own.wait()

        @pl.when(jnp.logical_not(own_slab))
        def _():
            give(0)[1].wait_recv()

    def gather(j, carry):
        project(unit(j, 0, core))

        @pl.when(j + 3 < count)
        def _():
            take(j + 3)

        @pl.when(j >= 1)
        def _():
            pass_on(j)

        u = unit(j, 0, 1 - core)
        arrive(u)
        project(u)
        for i in range(1, np_):
            project(unit(j, i, core))
        for i in range(1, np_):
            u = unit(j, i, 1 - core)
            arrive(u)
            project(u)
        return carry

    with jax.named_scope("gather"):
        lax.fori_loop(0, count, gather, 0)

    def send(s):
        return remote(
            mixed_heads.at[s], parts.at[slot], s_sem.at[s], a_sem.at[slot], s, mine
        )

    tile = min(512, blocks * block)
    tiles = blocks * block // tile

    def order(i):
        n = i // np_
        n = side * n + (1 - side) * (steps - 1 - n)
        return n * np_ + (share + 1 + i) % np_

    def score(i, h, n, top):
        at = pl.ds(pl.multiple_of(order(i) * block, block), block)
        keys = slice(n * tile, (n + 1) * tile)
        raw = lax.dot_general(
            k_ref[h, keys, :], q_ref[h, at, :], (((1,), (1,)), ((), ())),
            preferred_element_type=jnp.float32,
        )
        scores[h, keys, :] = raw
        return jnp.maximum(top, jnp.max(raw.reshape(tile // 8, 8, block), axis=0))

    def mix(h, n, top, total):
        keys = slice(n * tile, (n + 1) * tile)
        probs = jnp.exp2(scores[h, keys, :] - top).astype(jnp.bfloat16)
        return total + jnp.dot(v_ref[h, :, keys], probs, preferred_element_type=jnp.float32)

    lowest = jnp.full((8, block), -jnp.inf, jnp.float32)

    def attend_for(i, top):
        outs = []
        for h in range(heads):
            top = jnp.max(top, axis=0, keepdims=True)
            later = lowest
            total = jnp.zeros((v_ref.shape[1], block), jnp.float32)
            next_i, next_h = (i, h + 1) if h + 1 < heads else (jnp.minimum(i + 1, blocks - 1), 0)
            if heads == 1:
                for n in range(tiles):
                    total = mix(h, n, top, total)
                for n in range(tiles):
                    later = score(next_i, next_h, n, later)
            else:
                for n in range(tiles):
                    later = score(next_i, next_h, n, later)
                    total = mix(h, n, top, total)
            outs.append(total[:head_width] / total[head_width:head_width + 1])
            top = later
        s = order(i)
        mixed_heads[s] = jnp.concatenate(outs, axis=0).T.astype(jnp.bfloat16)
        kept = jnp.logical_and(home, s == b)

        @pl.when(jnp.logical_not(kept))
        def _():
            send(s).start()

        @pl.when(kept)
        def _():
            parts[slot] = mixed_heads[s]

        return top

    with jax.named_scope("attend"):
        top = lowest
        for n in range(tiles):
            top = score(0, 0, n, top)
        lax.fori_loop(0, blocks, attend_for, top)

    row = position * block + lax.broadcasted_iota(jnp.int32, (block, 128), 0)
    low = jnp.zeros((block, 128), jnp.int32)
    high = jnp.full((block, 128), blocks * groups * block, jnp.int32)
    for start in starts:
        low = jnp.where(row >= start, jnp.maximum(low, start), low)
        high = jnp.where(row < start, jnp.minimum(high, start), high)
    for t in range(taps):
        at = row + (t - half)
        masks[t] = jnp.where(jnp.logical_and(at >= low, at < high), 1.0, 0.0)

    with jax.named_scope("parts_wait"):
        for i in range(blocks):
            @pl.when(jnp.logical_not(jnp.logical_and(home, slot == i)))
            def _():
                remote(parts.at[i], parts.at[i], s_sem.at[i], a_sem.at[i], b, g).wait_recv()

    with jax.named_scope("mid_mm"):
        attended = jnp.concatenate([parts[i] for i in range(blocks)], axis=1)
        loads[0].wait()
        total = frames_ref[...].astype(jnp.float32) + jnp.dot(
            attended, w_out[...], preferred_element_type=jnp.float32
        )
        residual[...] = total.astype(jnp.bfloat16)
        conv_in = normalize(residual[...].astype(jnp.float32), conv_gain_ref[...]).astype(jnp.bfloat16)
        loads[1].wait()
        span = 256
        for n in range(0, width, span):
            a = jnp.dot(conv_in, w_glu[:, n:n + span], preferred_element_type=jnp.float32)
            gate = jnp.dot(
                conv_in, w_glu[:, width + n:width + n + span], preferred_element_type=jnp.float32
            )
            gated = (a * jax.nn.sigmoid(gate)).astype(jnp.bfloat16)
            edge[0, :, n:n + span] = gated[:rim]
            edge[1, :, n:n + span] = gated[block - rim:]
            for c in range(0, span, 128):
                extended[(n + c) // 128, rim:rim + block, :] = gated[:, c:c + 128].astype(jnp.float32)

    to_next = remote(
        edge.at[1], halo.at[0], hs_sem.at[1], hr_sem.at[0], after % blocks, after // blocks
    )
    to_prev = remote(
        edge.at[0], halo.at[1], hs_sem.at[0], hr_sem.at[1], before % blocks, before // blocks
    )
    to_next.start()
    to_prev.start()

    strip = min(64, block)
    spans = -(-taps // 8)

    def convolve(strips):
        def column(c, carry):
            cols = pl.ds(pl.multiple_of(c * 128, 128), 128)
            for r in strips:
                acc = jnp.zeros((strip, 128), jnp.float32)
                for p in range(8):
                    o = rim + r + p - half
                    slab = extended[c, o:o + strip + 8 * (spans - 1), :]
                    for j in range(spans):
                        t = 8 * j + p
                        if t < taps:
                            x = slab[8 * j:8 * j + strip] * masks[t, r:r + strip, :]
                            acc = acc + x * depth_ref[t:t + 1, cols]
                mixed[r:r + strip, cols] = acc
            return carry

        lax.fori_loop(0, width // 128, column, 0)

    every = list(range(0, block, strip))
    with jax.named_scope("conv_mid"):
        convolve(every[1:-1])
    with jax.named_scope("halo_wait"):
        to_next.wait_recv()
        to_prev.wait_recv()
    with jax.named_scope("conv_edge"):
        for c in range(width // 128):
            extended[c, :rim, :] = halo[0, :, 128 * c:128 * c + 128].astype(jnp.float32)
            extended[c, rim + block:2 * rim + block, :] = halo[1, :, 128 * c:128 * c + 128].astype(jnp.float32)
        convolve([every[0], every[-1]])
    with jax.named_scope("tail_mm"):
        normed = normalize(mixed[...], depth_gain_ref[...])
        activated = (normed * jax.nn.sigmoid(normed)).astype(jnp.bfloat16)
        loads[2].wait()
        out_ref[0] = (
            residual[...].astype(jnp.float32)
            + jnp.dot(activated, w_proj[...], preferred_element_type=jnp.float32)
        ).astype(out_ref.dtype)

    with jax.named_scope("drain"):
        for c in range(chunks):
            for k in range(parts_of_chunk):
                @pl.when(jnp.logical_not(self_kept))
                def _():
                    direct(c, k).wait_send()

        for other in range(groups):
            source, copy = give(other)

            @pl.when(jnp.logical_and(source == g, other != g))
            def _():
                copy.wait_send()

        def drain(j, carry):
            for k in range(parts_of_chunk):
                @pl.when(enters(j))
                def _():
                    for i in range(1, reach):
                        over(j, i, k).wait_send()

                for i in range(1, np_):
                    across(j, i, k).wait_send()
                for i in range(np_):
                    pair(j, i, k).wait_send()
            return carry

        lax.fori_loop(0, count, drain, 0)

        for i in range(blocks):
            @pl.when(jnp.logical_not(jnp.logical_and(home, b == i)))
            def _():
                send(i).wait_send()

        to_next.wait_send()
        to_prev.wait_send()


def body(
    frames, utt_lengths, attn_gain, w_qkv, w_out, conv_gain, w_glu, w_depth, depth_gain, w_proj
):
    rows, width = frames.shape[1:]
    blocks, groups = lax.axis_size("blk"), lax.axis_size("grp")
    head_width = width // HEADS
    np_ = blocks // groups
    columns = w_qkv.shape[1] // np_
    heads = columns // (3 * head_width)
    window = rows * blocks
    chunks = 2 if rows % 32 == 0 else 1
    parts_of_chunk = 2 if rows // chunks % 32 == 0 else 1
    reach = blocks // np_ // 2
    taps = w_depth.shape[0]
    rim = -(-(taps // 2) // 16) * 16
    vm = pl.BlockSpec(memory_space=pltpu.VMEM)
    hbm = pl.BlockSpec(memory_space=pl.ANY)
    return pl.pallas_call(
        functools.partial(block_kernel, blocks, groups, parts_of_chunk, head_width),
        out_shape=jax.ShapeDtypeStruct((1, rows, width), jnp.bfloat16),
        in_specs=[pl.BlockSpec(memory_space=pltpu.SMEM)] + [hbm] * 9,
        out_specs=vm,
        scratch_shapes=[
            pltpu.VMEM((rows, width), jnp.bfloat16),
            pltpu.VMEM((1, width), jnp.float32),
            pltpu.VMEM((1, width), jnp.float32),
            pltpu.VMEM(w_depth.shape, jnp.float32),
            pltpu.VMEM((1, width), jnp.float32),
            pltpu.VMEM((chunks, rows // chunks, width), jnp.bfloat16),
            pltpu.VMEM((blocks * chunks, rows // chunks, width), jnp.bfloat16),
            pltpu.VMEM((width, columns), jnp.bfloat16),
            pltpu.VMEM((width, columns), jnp.bfloat16),
            pltpu.VMEM((heads, window, 128), jnp.bfloat16),
            pltpu.VMEM((heads, window, 128), jnp.bfloat16),
            pltpu.VMEM((heads, head_width + 16, window), jnp.bfloat16),
            pltpu.VMEM((heads, window, rows), jnp.float32),
            pltpu.VMEM((blocks, rows, heads * head_width), jnp.bfloat16),
            pltpu.VMEM((blocks, rows, heads * head_width), jnp.bfloat16),
            pltpu.VMEM(w_out.shape, jnp.bfloat16),
            pltpu.VMEM(w_glu.shape, jnp.bfloat16),
            pltpu.VMEM(w_proj.shape, jnp.bfloat16),
            pltpu.VMEM((taps, rows, 128), jnp.float32),
            pltpu.VMEM((rows, width), jnp.bfloat16),
            pltpu.VMEM((2, rim, width), jnp.bfloat16),
            pltpu.VMEM((2, rim, width), jnp.bfloat16),
            pltpu.VMEM((width // 128, rows + 2 * rim + 8, 128), jnp.float32),
            pltpu.VMEM((rows, width), jnp.float32),
            pltpu.SemaphoreType.DMA((5,)),
            pltpu.SemaphoreType.DMA((5,)),
            pltpu.SemaphoreType.DMA((groups,)),
            pltpu.SemaphoreType.DMA((1,)),
            pltpu.SemaphoreType.DMA((chunks * parts_of_chunk,)),
            pltpu.SemaphoreType.DMA((reach * chunks * (reach - 1) * parts_of_chunk,)),
            pltpu.SemaphoreType.DMA((reach * chunks * np_ * parts_of_chunk,)),
            pltpu.SemaphoreType.DMA((reach * chunks * np_ * parts_of_chunk,)),
            pltpu.SemaphoreType.DMA((blocks * chunks * parts_of_chunk,)),
            pltpu.SemaphoreType.DMA((blocks,)),
            pltpu.SemaphoreType.DMA((blocks,)),
            pltpu.SemaphoreType.DMA((2,)),
            pltpu.SemaphoreType.DMA((2,)),
        ],
        compiler_params=pltpu.CompilerParams(
            collective_id=0, has_side_effects=True, vmem_limit_bytes=VMEM_LIMIT),
        name="block",
    )(
        utt_lengths, frames[0], attn_gain[None], conv_gain[None], w_depth, depth_gain[None],
        w_qkv, w_out, w_glu, w_proj,
    )


def solution(mesh):
    in_specs = (P("grp", "blk", None), P(), P(), P(None, "grp"), P(), P(), P(), P(), P(), P())
    out_specs = P("grp", "blk", None)
    return jax.shard_map(body, mesh=mesh, in_specs=in_specs, out_specs=out_specs, check_vma=False)
```

```python
import functools
import math

import jax
import jax.numpy as jnp
from jax import lax
from jax.experimental import pallas as pl
from jax.experimental.pallas import tpu as pltpu
from jax.sharding import PartitionSpec as P

HEADS = 16

epsilon = 1e-05
big_negative = -1e30
MESH = pl.DeviceIdType.MESH
VMEM_LIMIT = 56 * 1024 * 1024


def normalize(values, row_gain):
    center = values - jnp.mean(values, axis=-1, keepdims=True)
    spread = jnp.mean(center * center, axis=-1, keepdims=True)
    return center * lax.rsqrt(spread + epsilon) * row_gain


def starts_of(lengths_ref):
    starts, total = [], jnp.int32(0)
    for c in range(lengths_ref.shape[0]):
        starts.append(total)
        total = total + lengths_ref[c]
    return starts


def seg_at(starts, positions):
    seg = jnp.full(positions.shape, -1, jnp.int32)
    for start in starts:
        seg = seg + jnp.where(positions >= start, 1, 0)
    return seg


def remote(src, dst, send, recv, blk, grp):
    return pltpu.make_async_remote_copy(
        src_ref=src, dst_ref=dst, send_sem=send, recv_sem=recv,
        device_id=(blk, grp), device_id_type=MESH,
    )


def slot_of(b, g, blocks):
    half = blocks // 2
    return (b % half + (g % 2 + g // 2) * half) % blocks


def block_kernel(
    blocks, groups, parts_of_chunk, head_width,
    lengths_in, frames_in, gain_in, conv_gain_in, depth_in, depth_gain_in,
    w_ref, w_out_ref, w_glu_ref, w_proj_ref,
    out_ref,
    lengths_ref, frames_ref, gain_ref, conv_gain_ref, depth_ref, depth_gain_ref, norm, held, weights, lent, q_ref, k_ref, v_ref, scores,
    mixed_heads, parts, w_out, w_glu, w_proj, masks, residual, edge, halo, extended, mixed,
    load_sem, in_sem, ws_sem, wr_sem, d_sem, x_sem, y_sem, p_sem, r_sem, s_sem, a_sem, hs_sem, hr_sem,
):
    b, g = lax.axis_index("blk"), lax.axis_index("grp")
    np_ = blocks // groups
    steps = blocks // np_
    reach = steps // 2
    rows, width = held.shape[1:]
    chunks = norm.shape[0]
    block = rows * chunks
    part_rows = rows // parts_of_chunk
    columns = weights.shape[1]
    heads = columns // (3 * head_width)
    taps = depth_ref.shape[0]
    half = (taps - 1) // 2
    rim = halo.shape[1]
    step, share, core, chip = b // np_, b % np_, g % 2, g // 2
    side = step // reach
    mine = 2 * chip + side
    partner = g + 1 - 2 * core
    slot = slot_of(b, g, blocks)
    home = mine == g
    position = g * blocks + b

    last = blocks * groups - 1
    after = jnp.minimum(position + 1, last)
    before = jnp.maximum(position - 1, 0)
    has_after, has_before = position < last, position > 0
    barrier = pltpu.get_barrier_semaphore()

    def hail(other_b, other_g):
        pl.semaphore_signal(
            barrier, inc=1, device_id=(other_b, other_g), device_id_type=MESH
        )

    for c in range(2):
        def hail_row(i, carry):
            @pl.when(jnp.logical_or(i != b, core != c))
            def _():
                hail(i, 2 * chip + c)

            return carry

        lax.fori_loop(0, blocks, hail_row, 0)
    for other in range(groups):
        @pl.when(chip != other // 2)
        def _():
            hail(b, other)

    callers = 2 * blocks - 1 + groups - 2
    for near in (after, before):
        apart = near // blocks // 2 != chip

        @pl.when(apart)
        def _():
            hail(near % blocks, near // blocks)

        callers = callers + jnp.where(apart, 1, 0)

    inputs = [
        pltpu.make_async_copy(src, dst, in_sem.at[i]) for i, (src, dst) in enumerate([
            (frames_in, frames_ref), (gain_in, gain_ref), (conv_gain_in, conv_gain_ref),
            (depth_in, depth_ref), (depth_gain_in, depth_gain_ref), (lengths_in, lengths_ref),
        ])
    ]
    for copy in inputs:
        copy.start()

    def slab_of(sub):
        if np_ == 1:
            return w_ref
        return w_ref.at[:, pl.ds(pl.multiple_of(sub * columns, 128), columns)]

    own_slab = slot // np_ == g
    load_own = pltpu.make_async_copy(slab_of(b % np_), weights, load_sem.at[0])
    load_lent = pltpu.make_async_copy(slab_of(b % np_), lent, load_sem.at[4])

    def give(other):
        return slot_of(b, other, blocks) // np_, remote(
            lent, weights, ws_sem.at[other], wr_sem.at[0], b, other
        )

    @pl.when(own_slab)
    def _():
        load_own.start()

    load_lent.start()

    loads = [
        pltpu.make_async_copy(w_out_ref, w_out, load_sem.at[1]),
        pltpu.make_async_copy(w_glu_ref, w_glu, load_sem.at[2]),
        pltpu.make_async_copy(w_proj_ref, w_proj, load_sem.at[3]),
    ]

    def entry(n, at_side):
        first = at_side * reach
        return jnp.clip(n, first, first + reach - 1)

    target = entry(step, core) * np_ + share
    target_core = step % 2
    self_kept = jnp.logical_and(target == b, target_core == core)

    def piece(ref, u, k):
        return ref.at[u, pl.ds(k * part_rows, part_rows)]

    def direct(c, k):
        u = b * chunks + c
        return remote(
            piece(norm, c, k), piece(held, u, k), d_sem.at[c * parts_of_chunk + k], r_sem.at[u * parts_of_chunk + k],
            target, 2 * chip + target_core,
        )

    with jax.named_scope("in_wait"):
        for copy in inputs[:2]:
            copy.wait()
    with jax.named_scope("norm"):
        for c in range(chunks):
            part = frames_ref[c * rows:(c + 1) * rows, :].astype(jnp.float32)
            norm[c] = normalize(part, gain_ref[...]).astype(jnp.bfloat16)
    with jax.named_scope("barrier"):
        pl.semaphore_wait(barrier, callers)
    for c in range(chunks):
        for k in range(parts_of_chunk):
            at = slice(k * part_rows, (k + 1) * part_rows)

            @pl.when(jnp.logical_not(self_kept))
            def _():
                direct(c, k).start()

            @pl.when(self_kept)
            def _():
                held[b * chunks + c, at] = norm[c, at]

    for copy in inputs[2:]:
        copy.wait()
    load_lent.wait()
    for other in range(groups):
        source, copy = give(other)

        @pl.when(jnp.logical_and(source == g, other != g))
        def _():
            copy.start()

    for load in loads:
        load.start()

    lane = lax.broadcasted_iota(jnp.int32, (rows, 128), 1)
    row = lax.broadcasted_iota(jnp.int32, (rows, 128), 0)
    scale = head_width ** (-0.5) * math.log2(math.e)
    starts = starts_of(lengths_ref)

    for h in range(heads):
        at_row = lax.broadcasted_iota(jnp.int32, (16, v_ref.shape[2]), 0)
        v_ref[h, head_width:, :] = jnp.where(at_row == 0, 1.0, 0.0).astype(jnp.bfloat16)

    def padded(part):
        return jnp.concatenate([part, jnp.zeros((rows, 128 - head_width), jnp.float32)], axis=1)

    def project(u):
        out = jnp.dot(held[u], weights[...], preferred_element_type=jnp.float32)
        seg = seg_at(starts, mine * blocks * chunks * rows + u * rows + row)
        same = lane - head_width == seg
        at = pl.ds(pl.multiple_of(u * rows, rows), rows)
        for h in range(heads):
            o = 3 * head_width * h
            q = padded(out[:, o:o + head_width] * scale)
            k = padded(out[:, o + head_width:o + 2 * head_width])
            v = out[:, o + 2 * head_width:o + 3 * head_width]
            q = jnp.where(lane < head_width, q, jnp.where(same, big_negative, 0.0))
            k = jnp.where(lane < head_width, k, jnp.where(same, 0.0, 1.0))
            q_ref[h, at, :] = q.astype(jnp.bfloat16)
            k_ref[h, at, :] = k.astype(jnp.bfloat16)
            v_ref[h, :head_width, at] = v.T.astype(jnp.bfloat16)

    inner = step - side == reach - 1

    def unit(j, i, parity):
        swap = jnp.logical_and(inner, step % 2 != parity)
        n = jnp.where(swap, reach - 1 - j % reach, j // chunks)
        c = jnp.where(swap, j // reach, j % chunks)
        n = n + side * (reach - 1 - 2 * n)
        return ((2 * n + parity) * np_ + (share + i) % np_) * chunks + c

    def came(u, k):
        here = piece(held, u, k)
        return remote(here, here, p_sem.at[0], r_sem.at[u * parts_of_chunk + k], b, partner)

    def pair(j, i, k):
        u = unit(j, i, core)
        here = piece(held, u, k)
        return remote(
            here, here, p_sem.at[(j * np_ + i) * parts_of_chunk + k],
            r_sem.at[u * parts_of_chunk + k], b, partner,
        )

    def across(j, i, k):
        u = unit(j, 0, core)
        here = piece(held, u, k)
        return remote(
            here, here, y_sem.at[(j * np_ + i - 1) * parts_of_chunk + k],
            r_sem.at[u * parts_of_chunk + k], b - share + (share + i) % np_, g,
        )

    def over(j, i, k):
        u = unit(j, 0, core)
        here = piece(held, u, k)
        other = side * reach + (step - side * reach + i) % reach
        return remote(
            here, here, x_sem.at[(j * (reach - 1) + i - 1) * parts_of_chunk + k],
            r_sem.at[u * parts_of_chunk + k], other * np_ + share, g,
        )

    count = reach * chunks

    def enters(j):
        return entry(unit(j, 0, core) // (chunks * np_), side) == step

    def take(j):
        u = unit(j, 0, core)
        for k in range(parts_of_chunk):
            @pl.when(jnp.logical_not(jnp.logical_and(u // chunks == b, home)))
            def _():
                came(u, k).wait_recv()

            @pl.when(enters(j))
            def _():
                for i in range(1, reach):
                    over(j, i, k).start()

            for i in range(1, np_):
                across(j, i, k).start()
            pair(j, 0, k).start()

    def arrive(u):
        for k in range(parts_of_chunk):
            came(u, k).wait_recv()

    def pass_on(j):
        for i in range(1, np_):
            for k in range(parts_of_chunk):
                came(unit(j, i, core), k).wait_recv()
                pair(j, i, k).start()

    with jax.named_scope("first"):
        take(0)
        take(1)
        pass_on(0)
        if count > 2:
            take(2)

    with jax.named_scope("weights"):
        @pl.when(own_slab)
        def _():
            load_own.wait()

        @pl.when(jnp.logical_not(own_slab))
        def _():
            give(0)[1].wait_recv()

    def gather(j, carry):
        project(unit(j, 0, core))

        @pl.when(j + 3 < count)
        def _():
            take(j + 3)

        @pl.when(j >= 1)
        def _():
            pass_on(j)

        u = unit(j, 0, 1 - core)
        arrive(u)
        project(u)
        for i in range(1, np_):
            project(unit(j, i, core))
        for i in range(1, np_):
            u = unit(j, i, 1 - core)
            arrive(u)
            project(u)
        return carry

    with jax.named_scope("gather"):
        lax.fori_loop(0, count, gather, 0)

    def send(s):
        return remote(
            mixed_heads.at[s], parts.at[slot], s_sem.at[s], a_sem.at[slot], s, mine
        )

    tile = min(512, blocks * block)
    tiles = blocks * block // tile

    def order(i):
        far = jnp.logical_or(i == 0, jnp.logical_and(i % 2 == 1, i < blocks - 1))
        away = (i + 1) // 2
        close = jnp.where(i == blocks - 1, blocks // 2 - 1, i // 2 - 1)
        out_step = side * (away // np_) + (1 - side) * (steps - 1 - away // np_)
        in_step = side * reach + (step - side * reach + 1 + close // np_) % reach
        n = jnp.where(far, out_step, in_step)
        m = jnp.where(far, away, close)
        return n * np_ + (share + 1 + m) % np_

    def score(i, h, n, top):
        at = pl.ds(pl.multiple_of(order(i) * block, block), block)
        keys = slice(n * tile, (n + 1) * tile)
        raw = lax.dot_general(
            k_ref[h, keys, :], q_ref[h, at, :], (((1,), (1,)), ((), ())),
            preferred_element_type=jnp.float32,
        )
        scores[h, keys, :] = raw
        return jnp.maximum(top, jnp.max(raw.reshape(tile // 8, 8, block), axis=0))

    def mix(h, n, top, total):
        keys = slice(n * tile, (n + 1) * tile)
        probs = jnp.exp2(scores[h, keys, :] - top).astype(jnp.bfloat16)
        return total + jnp.dot(v_ref[h, :, keys], probs, preferred_element_type=jnp.float32)

    lowest = jnp.full((8, block), -jnp.inf, jnp.float32)

    def attend_for(i, top):
        outs = []
        for h in range(heads):
            top = jnp.max(top, axis=0, keepdims=True)
            later = lowest
            total = jnp.zeros((v_ref.shape[1], block), jnp.float32)
            next_i, next_h = (i, h + 1) if h + 1 < heads else (jnp.minimum(i + 1, blocks - 1), 0)
            if heads == 1:
                for n in range(tiles):
                    total = mix(h, n, top, total)
                for n in range(tiles):
                    later = score(next_i, next_h, n, later)
            else:
                for n in range(tiles):
                    later = score(next_i, next_h, n, later)
                    total = mix(h, n, top, total)
            outs.append(total[:head_width] / total[head_width:head_width + 1])
            top = later
        s = order(i)
        mixed_heads[s] = jnp.concatenate(outs, axis=0).T.astype(jnp.bfloat16)
        kept = jnp.logical_and(home, s == b)

        @pl.when(jnp.logical_not(kept))
        def _():
            send(s).start()

        @pl.when(kept)
        def _():
            parts[slot] = mixed_heads[s]

        return top

    with jax.named_scope("attend"):
        top = lowest
        for n in range(tiles):
            top = score(0, 0, n, top)
        lax.fori_loop(0, blocks, attend_for, top)

    row = position * block + lax.broadcasted_iota(jnp.int32, (block, 128), 0)
    low = jnp.zeros((block, 128), jnp.int32)
    high = jnp.full((block, 128), blocks * groups * block, jnp.int32)
    for start in starts:
        low = jnp.where(row >= start, jnp.maximum(low, start), low)
        high = jnp.where(row < start, jnp.minimum(high, start), high)
    for t in range(taps):
        at = row + (t - half)
        masks[t] = jnp.where(jnp.logical_and(at >= low, at < high), 1.0, 0.0)

    with jax.named_scope("parts_wait"):
        for i in range(blocks):
            @pl.when(jnp.logical_not(jnp.logical_and(home, slot == i)))
            def _():
                remote(parts.at[i], parts.at[i], s_sem.at[i], a_sem.at[i], b, g).wait_recv()

    with jax.named_scope("mid_mm"):
        attended = jnp.concatenate([parts[i] for i in range(blocks)], axis=1)
        loads[0].wait()
        total = frames_ref[...].astype(jnp.float32) + jnp.dot(
            attended, w_out[...], preferred_element_type=jnp.float32
        )
        residual[...] = total.astype(jnp.bfloat16)
        conv_in = normalize(residual[...].astype(jnp.float32), conv_gain_ref[...]).astype(jnp.bfloat16)
        loads[1].wait()
        span = 256
        for n in range(0, width, span):
            a = jnp.dot(conv_in, w_glu[:, n:n + span], preferred_element_type=jnp.float32)
            gate = jnp.dot(
                conv_in, w_glu[:, width + n:width + n + span], preferred_element_type=jnp.float32
            )
            gated = (a * jax.nn.sigmoid(gate)).astype(jnp.bfloat16)
            edge[0, :, n:n + span] = gated[:rim]
            edge[1, :, n:n + span] = gated[block - rim:]
            for c in range(0, span, 128):
                extended[(n + c) // 128, rim:rim + block, :] = gated[:, c:c + 128].astype(jnp.float32)

    to_next = remote(
        edge.at[1], halo.at[0], hs_sem.at[1], hr_sem.at[0], after % blocks, after // blocks
    )
    to_prev = remote(
        edge.at[0], halo.at[1], hs_sem.at[0], hr_sem.at[1], before % blocks, before // blocks
    )

    @pl.when(has_after)
    def _():
        to_next.start()

    @pl.when(has_before)
    def _():
        to_prev.start()

    strip = min(64, block)
    spans = -(-taps // 8)

    def convolve(strips):
        def column(c, carry):
            cols = pl.ds(pl.multiple_of(c * 128, 128), 128)
            for r in strips:
                acc = jnp.zeros((strip, 128), jnp.float32)
                for p in range(8):
                    o = rim + r + p - half
                    slab = extended[c, o:o + strip + 8 * (spans - 1), :]
                    for j in range(spans):
                        t = 8 * j + p
                        if t < taps:
                            x = slab[8 * j:8 * j + strip] * masks[t, r:r + strip, :]
                            acc = acc + x * depth_ref[t:t + 1, cols]
                mixed[r:r + strip, cols] = acc
            return carry

        lax.fori_loop(0, width // 128, column, 0)

    every = list(range(0, block, strip))
    with jax.named_scope("conv_mid"):
        convolve(every[1:-1])
    with jax.named_scope("halo_wait"):
        for i, present in ((0, has_before), (1, has_after)):
            @pl.when(present)
            def _():
                remote(
                    edge.at[i], halo.at[i], hs_sem.at[i], hr_sem.at[i], b, g
                ).wait_recv()

            @pl.when(jnp.logical_not(present))
            def _():
                halo[i] = jnp.zeros(halo.shape[1:], jnp.bfloat16)

    with jax.named_scope("conv_edge"):
        for c in range(width // 128):
            extended[c, :rim, :] = halo[0, :, 128 * c:128 * c + 128].astype(jnp.float32)
            extended[c, rim + block:2 * rim + block, :] = halo[1, :, 128 * c:128 * c + 128].astype(jnp.float32)
        convolve([every[0], every[-1]])
    with jax.named_scope("tail_mm"):
        normed = normalize(mixed[...], depth_gain_ref[...])
        activated = (normed * jax.nn.sigmoid(normed)).astype(jnp.bfloat16)
        loads[2].wait()
        out_ref[0] = (
            residual[...].astype(jnp.float32)
            + jnp.dot(activated, w_proj[...], preferred_element_type=jnp.float32)
        ).astype(out_ref.dtype)

    with jax.named_scope("drain"):
        for c in range(chunks):
            for k in range(parts_of_chunk):
                @pl.when(jnp.logical_not(self_kept))
                def _():
                    direct(c, k).wait_send()

        for other in range(groups):
            source, copy = give(other)

            @pl.when(jnp.logical_and(source == g, other != g))
            def _():
                copy.wait_send()

        def drain(j, carry):
            for k in range(parts_of_chunk):
                @pl.when(enters(j))
                def _():
                    for i in range(1, reach):
                        over(j, i, k).wait_send()

                for i in range(1, np_):
                    across(j, i, k).wait_send()
                for i in range(np_):
                    pair(j, i, k).wait_send()
            return carry

        lax.fori_loop(0, count, drain, 0)

        for i in range(blocks):
            @pl.when(jnp.logical_not(jnp.logical_and(home, b == i)))
            def _():
                send(i).wait_send()

        @pl.when(has_after)
        def _():
            to_next.wait_send()

        @pl.when(has_before)
        def _():
            to_prev.wait_send()


def body(
    frames, utt_lengths, attn_gain, w_qkv, w_out, conv_gain, w_glu, w_depth, depth_gain, w_proj
):
    rows, width = frames.shape[1:]
    blocks, groups = lax.axis_size("blk"), lax.axis_size("grp")
    head_width = width // HEADS
    np_ = blocks // groups
    columns = w_qkv.shape[1] // np_
    heads = columns // (3 * head_width)
    window = rows * blocks
    chunks = 2 if rows % 32 == 0 else 1
    parts_of_chunk = 2 if rows // chunks % 32 == 0 else 1
    reach = blocks // np_ // 2
    taps = w_depth.shape[0]
    rim = -(-(taps // 2) // 16) * 16
    vm = pl.BlockSpec(memory_space=pltpu.VMEM)
    hbm = pl.BlockSpec(memory_space=pl.ANY)
    return pl.pallas_call(
        functools.partial(block_kernel, blocks, groups, parts_of_chunk, head_width),
        out_shape=jax.ShapeDtypeStruct((1, rows, width), jnp.bfloat16),
        in_specs=[hbm] * 10,
        out_specs=vm,
        scratch_shapes=[
            pltpu.SMEM(utt_lengths.shape, jnp.int32),
            pltpu.VMEM((rows, width), jnp.bfloat16),
            pltpu.VMEM((1, width), jnp.float32),
            pltpu.VMEM((1, width), jnp.float32),
            pltpu.VMEM(w_depth.shape, jnp.float32),
            pltpu.VMEM((1, width), jnp.float32),
            pltpu.VMEM((chunks, rows // chunks, width), jnp.bfloat16),
            pltpu.VMEM((blocks * chunks, rows // chunks, width), jnp.bfloat16),
            pltpu.VMEM((width, columns), jnp.bfloat16),
            pltpu.VMEM((width, columns), jnp.bfloat16),
            pltpu.VMEM((heads, window, 128), jnp.bfloat16),
            pltpu.VMEM((heads, window, 128), jnp.bfloat16),
            pltpu.VMEM((heads, head_width + 16, window), jnp.bfloat16),
            pltpu.VMEM((heads, window, rows), jnp.float32),
            pltpu.VMEM((blocks, rows, heads * head_width), jnp.bfloat16),
            pltpu.VMEM((blocks, rows, heads * head_width), jnp.bfloat16),
            pltpu.VMEM(w_out.shape, jnp.bfloat16),
            pltpu.VMEM(w_glu.shape, jnp.bfloat16),
            pltpu.VMEM(w_proj.shape, jnp.bfloat16),
            pltpu.VMEM((taps, rows, 128), jnp.float32),
            pltpu.VMEM((rows, width), jnp.bfloat16),
            pltpu.VMEM((2, rim, width), jnp.bfloat16),
            pltpu.VMEM((2, rim, width), jnp.bfloat16),
            pltpu.VMEM((width // 128, rows + 2 * rim + 8, 128), jnp.float32),
            pltpu.VMEM((rows, width), jnp.float32),
            pltpu.SemaphoreType.DMA((5,)),
            pltpu.SemaphoreType.DMA((6,)),
            pltpu.SemaphoreType.DMA((groups,)),
            pltpu.SemaphoreType.DMA((1,)),
            pltpu.SemaphoreType.DMA((chunks * parts_of_chunk,)),
            pltpu.SemaphoreType.DMA((reach * chunks * (reach - 1) * parts_of_chunk,)),
            pltpu.SemaphoreType.DMA((reach * chunks * np_ * parts_of_chunk,)),
            pltpu.SemaphoreType.DMA((reach * chunks * np_ * parts_of_chunk,)),
            pltpu.SemaphoreType.DMA((blocks * chunks * parts_of_chunk,)),
            pltpu.SemaphoreType.DMA((blocks,)),
            pltpu.SemaphoreType.DMA((blocks,)),
            pltpu.SemaphoreType.DMA((2,)),
            pltpu.SemaphoreType.DMA((2,)),
        ],
        compiler_params=pltpu.CompilerParams(
            collective_id=0, has_side_effects=True, vmem_limit_bytes=VMEM_LIMIT),
        name="block",
    )(
        utt_lengths, frames[0], attn_gain[None], conv_gain[None], w_depth, depth_gain[None],
        w_qkv, w_out, w_glu, w_proj,
    )


def solution(mesh):
    in_specs = (P("grp", "blk", None), P(), P(), P(None, "grp"), P(), P(), P(), P(), P(), P())
    out_specs = P("grp", "blk", None)
    return jax.shard_map(body, mesh=mesh, in_specs=in_specs, out_specs=out_specs, check_vma=False)
```

```python
import functools
import math

import jax
import jax.numpy as jnp
from jax import lax
from jax.experimental import pallas as pl
from jax.experimental.pallas import tpu as pltpu
from jax.sharding import PartitionSpec as P

HEADS = 16

epsilon = 1e-05
big_negative = -1e30
MESH = pl.DeviceIdType.MESH
VMEM_LIMIT = 56 * 1024 * 1024


def normalize(values, row_gain):
    center = values - jnp.mean(values, axis=-1, keepdims=True)
    spread = jnp.mean(center * center, axis=-1, keepdims=True)
    return center * lax.rsqrt(spread + epsilon) * row_gain


def starts_of(lengths_ref):
    starts, total = [], jnp.int32(0)
    for c in range(lengths_ref.shape[0]):
        starts.append(total)
        total = total + lengths_ref[c]
    return starts


def seg_at(starts, positions):
    seg = jnp.full(positions.shape, -1, jnp.int32)
    for start in starts:
        seg = seg + jnp.where(positions >= start, 1, 0)
    return seg


def remote(src, dst, send, recv, blk, grp):
    return pltpu.make_async_remote_copy(
        src_ref=src, dst_ref=dst, send_sem=send, recv_sem=recv,
        device_id=(blk, grp), device_id_type=MESH,
    )


def finished(mixed, residual, row_gain, w_proj):
    normed = normalize(mixed, row_gain)
    activated = (normed * jax.nn.sigmoid(normed)).astype(jnp.bfloat16)
    return (
        residual.astype(jnp.float32)
        + jnp.dot(activated, w_proj, preferred_element_type=jnp.float32)
    ).astype(jnp.bfloat16)


def slot_of(b, g, blocks):
    half = blocks // 2
    return (b % half + (g % 2 + g // 2) * half) % blocks


def block_kernel(
    blocks, groups, parts_of_chunk, head_width,
    lengths_in, frames_in, gain_in, conv_gain_in, depth_in, depth_gain_in,
    w_ref, w_out_ref, w_glu_ref, w_proj_ref,
    out_ref,
    lengths_ref, frames_ref, gain_ref, conv_gain_ref, depth_ref, depth_gain_ref, norm, held, weights, lent, q_ref, k_ref, v_ref, scores,
    mixed_heads, parts, w_out, w_glu, w_proj, masks, residual, edge, halo, extended, mixed,
    load_sem, in_sem, ws_sem, wr_sem, d_sem, x_sem, y_sem, z_sem, p_sem, r_sem, s_sem, a_sem, hs_sem, hr_sem,
):
    b, g = lax.axis_index("blk"), lax.axis_index("grp")
    np_ = blocks // groups
    steps = blocks // np_
    reach = steps // 2
    rows, width = held.shape[1:]
    chunks = norm.shape[0]
    block = rows * chunks
    part_rows = rows // parts_of_chunk
    columns = weights.shape[1]
    heads = columns // (3 * head_width)
    taps = depth_ref.shape[0]
    half = (taps - 1) // 2
    rim = halo.shape[1]
    step, share, core, chip = b // np_, b % np_, g % 2, g // 2
    side = step // reach
    mine = 2 * chip + side
    partner = g + 1 - 2 * core
    slot = slot_of(b, g, blocks)
    home = mine == g
    position = g * blocks + b

    last = blocks * groups - 1
    after = jnp.minimum(position + 1, last)
    before = jnp.maximum(position - 1, 0)
    has_after, has_before = position < last, position > 0
    barrier = pltpu.get_barrier_semaphore()

    def hail(other_b, other_g):
        pl.semaphore_signal(
            barrier, inc=1, device_id=(other_b, other_g), device_id_type=MESH
        )

    for c in range(2):
        def hail_row(i, carry):
            @pl.when(jnp.logical_or(i != b, core != c))
            def _():
                hail(i, 2 * chip + c)

            return carry

        lax.fori_loop(0, blocks, hail_row, 0)
    for other in range(groups):
        @pl.when(chip != other // 2)
        def _():
            hail(b, other)

    callers = 2 * blocks - 1 + groups - 2
    for near in (after, before):
        apart = near // blocks // 2 != chip

        @pl.when(apart)
        def _():
            hail(near % blocks, near // blocks)

        callers = callers + jnp.where(apart, 1, 0)

    inputs = [
        pltpu.make_async_copy(src, dst, in_sem.at[i]) for i, (src, dst) in enumerate([
            (frames_in, frames_ref), (gain_in, gain_ref), (conv_gain_in, conv_gain_ref),
            (depth_in, depth_ref), (depth_gain_in, depth_gain_ref), (lengths_in, lengths_ref),
        ])
    ]
    for copy in inputs:
        copy.start()

    def slab_of(sub):
        if np_ == 1:
            return w_ref
        return w_ref.at[:, pl.ds(pl.multiple_of(sub * columns, 128), columns)]

    own_slab = slot // np_ == g
    load_own = pltpu.make_async_copy(slab_of(b % np_), weights, load_sem.at[0])
    load_lent = pltpu.make_async_copy(slab_of(b % np_), lent, load_sem.at[4])

    def give(other):
        return slot_of(b, other, blocks) // np_, remote(
            lent, weights, ws_sem.at[other], wr_sem.at[0], b, other
        )

    @pl.when(own_slab)
    def _():
        load_own.start()

    load_lent.start()

    loads = [
        pltpu.make_async_copy(w_out_ref, w_out, load_sem.at[1]),
        pltpu.make_async_copy(w_glu_ref, w_glu, load_sem.at[2]),
        pltpu.make_async_copy(w_proj_ref, w_proj, load_sem.at[3]),
    ]

    def entry(n, at_side):
        first = at_side * reach
        return jnp.clip(n, first, first + reach - 1)

    target = entry(step, core) * np_ + share
    target_core = step % 2
    self_kept = jnp.logical_and(target == b, target_core == core)

    def piece(ref, u, k):
        return ref.at[u, pl.ds(k * part_rows, part_rows)]

    def direct(c, k):
        u = b * chunks + c
        return remote(
            piece(norm, c, k), piece(held, u, k), d_sem.at[c * parts_of_chunk + k], r_sem.at[u * parts_of_chunk + k],
            target, 2 * chip + target_core,
        )

    with jax.named_scope("in_wait"):
        for copy in inputs[:2]:
            copy.wait()
    with jax.named_scope("norm"):
        for c in range(chunks):
            part = frames_ref[c * rows:(c + 1) * rows, :].astype(jnp.float32)
            norm[c] = normalize(part, gain_ref[...]).astype(jnp.bfloat16)
    with jax.named_scope("barrier"):
        pl.semaphore_wait(barrier, callers)
    for c in range(chunks):
        for k in range(parts_of_chunk):
            at = slice(k * part_rows, (k + 1) * part_rows)

            @pl.when(jnp.logical_not(self_kept))
            def _():
                direct(c, k).start()

            @pl.when(self_kept)
            def _():
                held[b * chunks + c, at] = norm[c, at]

    for copy in inputs[2:]:
        copy.wait()
    load_lent.wait()
    for other in range(groups):
        source, copy = give(other)

        @pl.when(jnp.logical_and(source == g, other != g))
        def _():
            copy.start()

    for load in loads:
        load.start()

    lane = lax.broadcasted_iota(jnp.int32, (rows, 128), 1)
    row = lax.broadcasted_iota(jnp.int32, (rows, 128), 0)
    scale = head_width ** (-0.5) * math.log2(math.e)
    starts = starts_of(lengths_ref)

    for h in range(heads):
        at_row = lax.broadcasted_iota(jnp.int32, (16, v_ref.shape[2]), 0)
        v_ref[h, head_width:, :] = jnp.where(at_row == 0, 1.0, 0.0).astype(jnp.bfloat16)

    def padded(part):
        return jnp.concatenate([part, jnp.zeros((rows, 128 - head_width), jnp.float32)], axis=1)

    def project(u):
        out = jnp.dot(held[u], weights[...], preferred_element_type=jnp.float32)
        seg = seg_at(starts, mine * blocks * chunks * rows + u * rows + row)
        same = lane - head_width == seg
        at = pl.ds(pl.multiple_of(u * rows, rows), rows)
        for h in range(heads):
            o = 3 * head_width * h
            q = padded(out[:, o:o + head_width] * scale)
            k = padded(out[:, o + head_width:o + 2 * head_width])
            v = out[:, o + 2 * head_width:o + 3 * head_width]
            q = jnp.where(lane < head_width, q, jnp.where(same, big_negative, 0.0))
            k = jnp.where(lane < head_width, k, jnp.where(same, 0.0, 1.0))
            q_ref[h, at, :] = q.astype(jnp.bfloat16)
            k_ref[h, at, :] = k.astype(jnp.bfloat16)
            v_ref[h, :head_width, at] = v.T.astype(jnp.bfloat16)

    inner = step - side == reach - 1

    def unit(j, i, parity):
        swap = jnp.logical_and(inner, step % 2 != parity)
        n = jnp.where(swap, reach - 1 - j % reach, j // chunks)
        c = jnp.where(swap, j // reach, j % chunks)
        n = n + side * (reach - 1 - 2 * n)
        return ((2 * n + parity) * np_ + (share + i) % np_) * chunks + c

    lifts = reach == 2 and np_ > 1
    inner_step, outer_step = reach - 1 + side, side * (steps - 1)

    def lifted(u, at_inner):
        return jnp.logical_and(at_inner, u // (chunks * np_) == outer_step)

    def lift(j, i, k):
        u = unit(j, i, core)
        here = piece(held, u, k)
        return remote(
            here, here, z_sem.at[(j * (np_ - 1) + i - 1) * parts_of_chunk + k],
            r_sem.at[u * parts_of_chunk + k],
            (side * reach + (step - side * reach + 1) % reach) * np_ + share, g,
        )

    def crosses(j):
        if lifts:
            return jnp.logical_not(lifted(unit(j, 0, core), inner))
        return j >= 0

    def climbs(j, i):
        return lifted(unit(j, i, core), jnp.logical_not(inner))

    early = jnp.logical_and(step == outer_step, step % 2 == core)

    def came(u, k):
        here = piece(held, u, k)
        return remote(here, here, p_sem.at[0], r_sem.at[u * parts_of_chunk + k], b, partner)

    def pair(j, i, k):
        u = unit(j, i, core)
        here = piece(held, u, k)
        return remote(
            here, here, p_sem.at[(j * np_ + i) * parts_of_chunk + k],
            r_sem.at[u * parts_of_chunk + k], b, partner,
        )

    def across(j, i, k):
        u = unit(j, 0, core)
        here = piece(held, u, k)
        return remote(
            here, here, y_sem.at[(j * (np_ - 1) + i - 1) * parts_of_chunk + k],
            r_sem.at[u * parts_of_chunk + k], b - share + (share + i) % np_, g,
        )

    def over(j, i, k):
        u = unit(j, 0, core)
        here = piece(held, u, k)
        other = side * reach + (step - side * reach + i) % reach
        return remote(
            here, here, x_sem.at[(j * (reach - 1) + i - 1) * parts_of_chunk + k],
            r_sem.at[u * parts_of_chunk + k], other * np_ + share, g,
        )

    count = reach * chunks

    def enters(j):
        return entry(unit(j, 0, core) // (chunks * np_), side) == step

    def take(j):
        u = unit(j, 0, core)
        for k in range(parts_of_chunk):
            @pl.when(jnp.logical_not(jnp.logical_and(u // chunks == b, home)))
            def _():
                came(u, k).wait_recv()

            @pl.when(enters(j))
            def _():
                for i in range(1, reach):
                    over(j, i, k).start()

            @pl.when(crosses(j))
            def _():
                for i in range(1, np_):
                    across(j, i, k).start()

            pair(j, 0, k).start()

    def arrive(u):
        for k in range(parts_of_chunk):
            came(u, k).wait_recv()

    def pass_on(j):
        for i in range(1, np_):
            for k in range(parts_of_chunk):
                came(unit(j, i, core), k).wait_recv()
                if lifts:
                    @pl.when(climbs(j, i))
                    def _():
                        lift(j, i, k).start()

                pair(j, i, k).start()

    with jax.named_scope("first"):
        take(0)
        take(1)
        pass_on(0)

        @pl.when(early)
        def _():
            pass_on(1)

        if count > 2:
            take(2)

    with jax.named_scope("weights"):
        @pl.when(own_slab)
        def _():
            load_own.wait()

        @pl.when(jnp.logical_not(own_slab))
        def _():
            give(0)[1].wait_recv()

    def gather(j, carry):
        project(unit(j, 0, core))

        @pl.when(j + 3 < count)
        def _():
            take(j + 3)

        @pl.when(jnp.logical_or(j >= 2, jnp.logical_and(j == 1, jnp.logical_not(early))))
        def _():
            pass_on(j)

        u = unit(j, 0, 1 - core)
        arrive(u)
        project(u)
        for i in range(1, np_):
            project(unit(j, i, core))
        for i in range(1, np_):
            u = unit(j, i, 1 - core)
            arrive(u)
            project(u)
        return carry

    with jax.named_scope("gather"):
        lax.fori_loop(0, count, gather, 0)

    def send(s):
        return remote(
            mixed_heads.at[s], parts.at[slot], s_sem.at[s], a_sem.at[slot], s, mine
        )

    tile = min(512, blocks * block)
    tiles = blocks * block // tile

    def order(i):
        far = jnp.logical_or(i == 0, jnp.logical_and(i % 2 == 1, i < blocks - 1))
        away = (i + 1) // 2
        close = jnp.where(i == blocks - 1, blocks // 2 - 1, i // 2 - 1)
        out_step = side * (away // np_) + (1 - side) * (steps - 1 - away // np_)
        in_step = side * reach + (step - side * reach + 1 + close // np_) % reach
        n = jnp.where(far, out_step, in_step)
        m = jnp.where(far, away, close)
        return n * np_ + (share + 1 + m) % np_

    def score(i, h, n, top):
        at = pl.ds(pl.multiple_of(order(i) * block, block), block)
        keys = slice(n * tile, (n + 1) * tile)
        raw = lax.dot_general(
            k_ref[h, keys, :], q_ref[h, at, :], (((1,), (1,)), ((), ())),
            preferred_element_type=jnp.float32,
        )
        scores[h, keys, :] = raw
        return jnp.maximum(top, jnp.max(raw.reshape(tile // 8, 8, block), axis=0))

    def mix(h, n, top, total):
        keys = slice(n * tile, (n + 1) * tile)
        probs = jnp.exp2(scores[h, keys, :] - top).astype(jnp.bfloat16)
        return total + jnp.dot(v_ref[h, :, keys], probs, preferred_element_type=jnp.float32)

    lowest = jnp.full((8, block), -jnp.inf, jnp.float32)

    def attend_for(i, top):
        outs = []
        for h in range(heads):
            top = jnp.max(top, axis=0, keepdims=True)
            later = lowest
            total = jnp.zeros((v_ref.shape[1], block), jnp.float32)
            next_i, next_h = (i, h + 1) if h + 1 < heads else (jnp.minimum(i + 1, blocks - 1), 0)
            if heads == 1:
                for n in range(tiles):
                    total = mix(h, n, top, total)
                for n in range(tiles):
                    later = score(next_i, next_h, n, later)
            else:
                for n in range(tiles):
                    later = score(next_i, next_h, n, later)
                    total = mix(h, n, top, total)
            outs.append(total[:head_width] / total[head_width:head_width + 1])
            top = later
        s = order(i)
        mixed_heads[s] = jnp.concatenate(outs, axis=0).T.astype(jnp.bfloat16)
        kept = jnp.logical_and(home, s == b)

        @pl.when(jnp.logical_not(kept))
        def _():
            send(s).start()

        @pl.when(kept)
        def _():
            parts[slot] = mixed_heads[s]

        return top

    with jax.named_scope("attend"):
        top = lowest
        for n in range(tiles):
            top = score(0, 0, n, top)
        lax.fori_loop(0, blocks, attend_for, top)

    row = position * block + lax.broadcasted_iota(jnp.int32, (block, 128), 0)
    low = jnp.zeros((block, 128), jnp.int32)
    high = jnp.full((block, 128), blocks * groups * block, jnp.int32)
    for start in starts:
        low = jnp.where(row >= start, jnp.maximum(low, start), low)
        high = jnp.where(row < start, jnp.minimum(high, start), high)
    for t in range(taps):
        at = row + (t - half)
        masks[t] = jnp.where(jnp.logical_and(at >= low, at < high), 1.0, 0.0)

    part_width = parts.shape[2]
    together = max(1, 256 // part_width)
    with jax.named_scope("parts_wait"):
        loads[0].wait()
        total = frames_ref[...].astype(jnp.float32)
        for first in range(0, blocks, together):
            for i in range(first, first + together):
                @pl.when(jnp.logical_not(jnp.logical_and(home, slot == i)))
                def _():
                    remote(parts.at[i], parts.at[i], s_sem.at[i], a_sem.at[i], b, g).wait_recv()

            attended = jnp.concatenate([parts[first + i] for i in range(together)], axis=1)
            at = slice(first * part_width, (first + together) * part_width)
            total = total + jnp.dot(attended, w_out[at, :], preferred_element_type=jnp.float32)
            if first + together < blocks:
                mixed[...] = total
                total = mixed[...]

    with jax.named_scope("mid_mm"):
        residual[...] = total.astype(jnp.bfloat16)
        conv_in = normalize(residual[...].astype(jnp.float32), conv_gain_ref[...]).astype(jnp.bfloat16)
        loads[1].wait()
        span = 256
        for n in range(0, width, span):
            a = jnp.dot(conv_in, w_glu[:, n:n + span], preferred_element_type=jnp.float32)
            gate = jnp.dot(
                conv_in, w_glu[:, width + n:width + n + span], preferred_element_type=jnp.float32
            )
            gated = (a * jax.nn.sigmoid(gate)).astype(jnp.bfloat16)
            edge[0, :, n:n + span] = gated[:rim]
            edge[1, :, n:n + span] = gated[block - rim:]
            for c in range(0, span, 128):
                extended[(n + c) // 128, rim:rim + block, :] = gated[:, c:c + 128].astype(jnp.float32)

    to_next = remote(
        edge.at[1], halo.at[0], hs_sem.at[1], hr_sem.at[0], after % blocks, after // blocks
    )
    to_prev = remote(
        edge.at[0], halo.at[1], hs_sem.at[0], hr_sem.at[1], before % blocks, before // blocks
    )

    @pl.when(has_after)
    def _():
        to_next.start()

    @pl.when(has_before)
    def _():
        to_prev.start()

    spans = -(-taps // 8)

    def convolve(strips):
        def column(c, carry):
            cols = pl.ds(pl.multiple_of(c * 128, 128), 128)
            for r, strip in strips:
                acc = jnp.zeros((strip, 128), jnp.float32)
                for p in range(8):
                    o = rim + r + p - half
                    slab = extended[c, o:o + strip + 8 * (spans - 1), :]
                    for t in range(p, taps, 8):
                        x = slab[t - p:t - p + strip] * masks[t, r:r + strip, :]
                        acc = acc + x * depth_ref[t:t + 1, cols]
                mixed[r:r + strip, cols] = acc
            return carry

        lax.fori_loop(0, width // 128, column, 0)

    with jax.named_scope("conv_mid"):
        convolve([(r, min(64, block - rim - r)) for r in range(rim, block - rim, 64)])
    with jax.named_scope("tail_mm"):
        loads[2].wait()
        out_ref[0, rim:block - rim] = finished(
            mixed[rim:block - rim], residual[rim:block - rim], depth_gain_ref[...], w_proj[...]
        )
    with jax.named_scope("halo_wait"):
        for i, present in ((0, has_before), (1, has_after)):
            @pl.when(present)
            def _():
                remote(
                    edge.at[i], halo.at[i], hs_sem.at[i], hr_sem.at[i], b, g
                ).wait_recv()

            @pl.when(jnp.logical_not(present))
            def _():
                halo[i] = jnp.zeros(halo.shape[1:], jnp.bfloat16)

    with jax.named_scope("conv_edge"):
        for c in range(width // 128):
            at = slice(128 * c, 128 * c + 128)
            extended[c, :rim, :] = halo[0, :, at].astype(jnp.float32)
            extended[c, rim + block:2 * rim + block, :] = halo[1, :, at].astype(jnp.float32)
        convolve([(0, rim), (block - rim, rim)])
    with jax.named_scope("tail_edge"):
        ends = finished(
            jnp.concatenate([mixed[:rim], mixed[block - rim:]], axis=0),
            jnp.concatenate([residual[:rim], residual[block - rim:]], axis=0),
            depth_gain_ref[...], w_proj[...],
        )
        out_ref[0, :rim] = ends[:rim]
        out_ref[0, block - rim:] = ends[rim:]

    with jax.named_scope("drain"):
        for c in range(chunks):
            for k in range(parts_of_chunk):
                @pl.when(jnp.logical_not(self_kept))
                def _():
                    direct(c, k).wait_send()

        for other in range(groups):
            source, copy = give(other)

            @pl.when(jnp.logical_and(source == g, other != g))
            def _():
                copy.wait_send()

        def drain(j, carry):
            for k in range(parts_of_chunk):
                @pl.when(enters(j))
                def _():
                    for i in range(1, reach):
                        over(j, i, k).wait_send()

                @pl.when(crosses(j))
                def _():
                    for i in range(1, np_):
                        across(j, i, k).wait_send()

                if lifts:
                    for i in range(1, np_):
                        @pl.when(climbs(j, i))
                        def _():
                            lift(j, i, k).wait_send()

                for i in range(np_):
                    pair(j, i, k).wait_send()
            return carry

        lax.fori_loop(0, count, drain, 0)

        for i in range(blocks):
            @pl.when(jnp.logical_not(jnp.logical_and(home, b == i)))
            def _():
                send(i).wait_send()

        @pl.when(has_after)
        def _():
            to_next.wait_send()

        @pl.when(has_before)
        def _():
            to_prev.wait_send()


def body(
    frames, utt_lengths, attn_gain, w_qkv, w_out, conv_gain, w_glu, w_depth, depth_gain, w_proj
):
    rows, width = frames.shape[1:]
    blocks, groups = lax.axis_size("blk"), lax.axis_size("grp")
    head_width = width // HEADS
    np_ = blocks // groups
    columns = w_qkv.shape[1] // np_
    heads = columns // (3 * head_width)
    window = rows * blocks
    chunks = 2 if rows % 32 == 0 else 1
    parts_of_chunk = 2 if rows // chunks % 32 == 0 else 1
    reach = blocks // np_ // 2
    taps = w_depth.shape[0]
    rim = -(-(taps // 2) // 16) * 16
    vm = pl.BlockSpec(memory_space=pltpu.VMEM)
    hbm = pl.BlockSpec(memory_space=pl.ANY)
    return pl.pallas_call(
        functools.partial(block_kernel, blocks, groups, parts_of_chunk, head_width),
        out_shape=jax.ShapeDtypeStruct((1, rows, width), jnp.bfloat16),
        in_specs=[hbm] * 10,
        out_specs=vm,
        scratch_shapes=[
            pltpu.SMEM(utt_lengths.shape, jnp.int32),
            pltpu.VMEM((rows, width), jnp.bfloat16),
            pltpu.VMEM((1, width), jnp.float32),
            pltpu.VMEM((1, width), jnp.float32),
            pltpu.VMEM(w_depth.shape, jnp.float32),
            pltpu.VMEM((1, width), jnp.float32),
            pltpu.VMEM((chunks, rows // chunks, width), jnp.bfloat16),
            pltpu.VMEM((blocks * chunks, rows // chunks, width), jnp.bfloat16),
            pltpu.VMEM((width, columns), jnp.bfloat16),
            pltpu.VMEM((width, columns), jnp.bfloat16),
            pltpu.VMEM((heads, window, 128), jnp.bfloat16),
            pltpu.VMEM((heads, window, 128), jnp.bfloat16),
            pltpu.VMEM((heads, head_width + 16, window), jnp.bfloat16),
            pltpu.VMEM((heads, window, rows), jnp.float32),
            pltpu.VMEM((blocks, rows, heads * head_width), jnp.bfloat16),
            pltpu.VMEM((blocks, rows, heads * head_width), jnp.bfloat16),
            pltpu.VMEM(w_out.shape, jnp.bfloat16),
            pltpu.VMEM(w_glu.shape, jnp.bfloat16),
            pltpu.VMEM(w_proj.shape, jnp.bfloat16),
            pltpu.VMEM((taps, rows, 128), jnp.float32),
            pltpu.VMEM((rows, width), jnp.bfloat16),
            pltpu.VMEM((2, rim, width), jnp.bfloat16),
            pltpu.VMEM((2, rim, width), jnp.bfloat16),
            pltpu.VMEM((width // 128, rows + 2 * rim + 8, 128), jnp.float32),
            pltpu.VMEM((rows, width), jnp.float32),
            pltpu.SemaphoreType.DMA((5,)),
            pltpu.SemaphoreType.DMA((6,)),
            pltpu.SemaphoreType.DMA((groups,)),
            pltpu.SemaphoreType.DMA((1,)),
            pltpu.SemaphoreType.DMA((chunks * parts_of_chunk,)),
            pltpu.SemaphoreType.DMA((reach * chunks * (reach - 1) * parts_of_chunk,)),
            pltpu.SemaphoreType.DMA((reach * chunks * max(np_ - 1, 1) * parts_of_chunk,)),
            pltpu.SemaphoreType.DMA((reach * chunks * max(np_ - 1, 1) * parts_of_chunk,)),
            pltpu.SemaphoreType.DMA((reach * chunks * np_ * parts_of_chunk,)),
            pltpu.SemaphoreType.DMA((blocks * chunks * parts_of_chunk,)),
            pltpu.SemaphoreType.DMA((blocks,)),
            pltpu.SemaphoreType.DMA((blocks,)),
            pltpu.SemaphoreType.DMA((2,)),
            pltpu.SemaphoreType.DMA((2,)),
        ],
        compiler_params=pltpu.CompilerParams(
            collective_id=0, has_side_effects=True, vmem_limit_bytes=VMEM_LIMIT),
        name="block",
    )(
        utt_lengths, frames[0], attn_gain[None], conv_gain[None], w_depth, depth_gain[None],
        w_qkv, w_out, w_glu, w_proj,
    )


def solution(mesh):
    in_specs = (P("grp", "blk", None), P(), P(), P(None, "grp"), P(), P(), P(), P(), P(), P())
    out_specs = P("grp", "blk", None)
    return jax.shard_map(body, mesh=mesh, in_specs=in_specs, out_specs=out_specs, check_vma=False)
```

```python
import functools
import math

import jax
import jax.numpy as jnp
from jax import lax
from jax.experimental import pallas as pl
from jax.experimental.pallas import tpu as pltpu
from jax.sharding import PartitionSpec as P

HEADS = 16

epsilon = 1e-05
big_negative = -1e30
MESH = pl.DeviceIdType.MESH
VMEM_LIMIT = 56 * 1024 * 1024


def normalize(values, row_gain):
    center = values - jnp.mean(values, axis=-1, keepdims=True)
    spread = jnp.mean(center * center, axis=-1, keepdims=True)
    return center * lax.rsqrt(spread + epsilon) * row_gain


def starts_of(lengths_ref):
    starts, total = [], jnp.int32(0)
    for c in range(lengths_ref.shape[0]):
        starts.append(total)
        total = total + lengths_ref[c]
    return starts


def seg_at(starts, positions):
    seg = jnp.full(positions.shape, -1, jnp.int32)
    for start in starts:
        seg = seg + jnp.where(positions >= start, 1, 0)
    return seg


def remote(src, dst, send, recv, blk, grp):
    return pltpu.make_async_remote_copy(
        src_ref=src, dst_ref=dst, send_sem=send, recv_sem=recv,
        device_id=(blk, grp), device_id_type=MESH,
    )


def finished(mixed, residual, row_gain, w_proj):
    normed = normalize(mixed, row_gain)
    activated = (normed * jax.nn.sigmoid(normed)).astype(jnp.bfloat16)
    return (
        residual.astype(jnp.float32)
        + jnp.dot(activated, w_proj, preferred_element_type=jnp.float32)
    ).astype(jnp.bfloat16)


def slot_of(b, g, blocks):
    half = blocks // 2
    return (b % half + (g % 2 + g // 2) * half) % blocks


def block_kernel(
    blocks, groups, parts_of_chunk, head_width,
    lengths_in, frames_in, gain_in, conv_gain_in, depth_in, depth_gain_in,
    w_ref, w_out_ref, w_glu_ref, w_proj_ref,
    out_ref,
    lengths_ref, frames_ref, gain_ref, conv_gain_ref, depth_ref, depth_gain_ref, norm, held, weights, lent, q_ref, k_ref, v_ref, scores,
    mixed_heads, parts, w_out, w_glu, w_proj, masks, residual, edge, halo, extended, mixed,
    load_sem, in_sem, ws_sem, wr_sem, d_sem, x_sem, y_sem, z_sem, p_sem, r_sem, s_sem, a_sem, hs_sem, hr_sem,
):
    b, g = lax.axis_index("blk"), lax.axis_index("grp")
    np_ = blocks // groups
    steps = blocks // np_
    reach = steps // 2
    rows, width = held.shape[1:]
    chunks = norm.shape[0]
    block = rows * chunks
    part_rows = rows // parts_of_chunk
    columns = weights.shape[1]
    heads = columns // (3 * head_width)
    taps = depth_ref.shape[0]
    half = (taps - 1) // 2
    rim = halo.shape[1]
    step, share, core, chip = b // np_, b % np_, g % 2, g // 2
    side = step // reach
    mine = 2 * chip + side
    partner = g + 1 - 2 * core
    slot = slot_of(b, g, blocks)
    home = mine == g
    position = g * blocks + b

    last = blocks * groups - 1
    after = jnp.minimum(position + 1, last)
    before = jnp.maximum(position - 1, 0)
    has_after, has_before = position < last, position > 0
    barrier = pltpu.get_barrier_semaphore()

    def hail(other_b, other_g):
        pl.semaphore_signal(
            barrier, inc=1, device_id=(other_b, other_g), device_id_type=MESH
        )

    for c in range(2):
        def hail_row(i, carry):
            @pl.when(jnp.logical_or(i != b, core != c))
            def _():
                hail(i, 2 * chip + c)

            return carry

        lax.fori_loop(0, blocks, hail_row, 0)
    for other in range(groups):
        @pl.when(chip != other // 2)
        def _():
            hail(b, other)

    callers = 2 * blocks - 1 + groups - 2
    for near in (after, before):
        apart = near // blocks // 2 != chip

        @pl.when(apart)
        def _():
            hail(near % blocks, near // blocks)

        callers = callers + jnp.where(apart, 1, 0)

    inputs = [
        pltpu.make_async_copy(src, dst, in_sem.at[i]) for i, (src, dst) in enumerate([
            (frames_in, frames_ref), (gain_in, gain_ref), (conv_gain_in, conv_gain_ref),
            (depth_in, depth_ref), (depth_gain_in, depth_gain_ref), (lengths_in, lengths_ref),
        ])
    ]
    for copy in inputs:
        copy.start()

    def slab_of(sub):
        if np_ == 1:
            return w_ref
        return w_ref.at[:, pl.ds(pl.multiple_of(sub * columns, 128), columns)]

    own_slab = slot // np_ == g
    load_own = pltpu.make_async_copy(slab_of(b % np_), weights, load_sem.at[0])
    load_lent = pltpu.make_async_copy(slab_of(b % np_), lent, load_sem.at[4])

    def give(other):
        return slot_of(b, other, blocks) // np_, remote(
            lent, weights, ws_sem.at[other], wr_sem.at[0], b, other
        )

    @pl.when(own_slab)
    def _():
        load_own.start()

    load_lent.start()

    loads = [
        pltpu.make_async_copy(w_out_ref, w_out, load_sem.at[1]),
        pltpu.make_async_copy(w_glu_ref, w_glu, load_sem.at[2]),
        pltpu.make_async_copy(w_proj_ref, w_proj, load_sem.at[3]),
    ]

    def entry(n, at_side):
        first = at_side * reach
        return jnp.clip(n, first, first + reach - 1)

    target = entry(step, core) * np_ + share
    target_core = step % 2
    self_kept = jnp.logical_and(target == b, target_core == core)

    def piece(ref, u, k):
        return ref.at[u, pl.ds(k * part_rows, part_rows)]

    def direct(c, k):
        u = b * chunks + c
        return remote(
            piece(norm, c, k), piece(held, u, k), d_sem.at[c * parts_of_chunk + k], r_sem.at[u * parts_of_chunk + k],
            target, 2 * chip + target_core,
        )

    with jax.named_scope("in_wait"):
        for copy in inputs[:2]:
            copy.wait()
    with jax.named_scope("norm"):
        for c in range(chunks):
            part = frames_ref[c * rows:(c + 1) * rows, :].astype(jnp.float32)
            norm[c] = normalize(part, gain_ref[...]).astype(jnp.bfloat16)
    with jax.named_scope("barrier"):
        pl.semaphore_wait(barrier, callers)
    for c in range(chunks):
        for k in range(parts_of_chunk):
            at = slice(k * part_rows, (k + 1) * part_rows)

            @pl.when(jnp.logical_not(self_kept))
            def _():
                direct(c, k).start()

            @pl.when(self_kept)
            def _():
                held[b * chunks + c, at] = norm[c, at]

    for copy in inputs[2:]:
        copy.wait()
    load_lent.wait()
    for other in range(groups):
        source, copy = give(other)

        @pl.when(jnp.logical_and(source == g, other != g))
        def _():
            copy.start()

    for load in loads:
        load.start()

    lane = lax.broadcasted_iota(jnp.int32, (rows, 128), 1)
    row = lax.broadcasted_iota(jnp.int32, (rows, 128), 0)
    scale = head_width ** (-0.5) * math.log2(math.e)
    starts = starts_of(lengths_ref)

    for h in range(heads):
        at_row = lax.broadcasted_iota(jnp.int32, (16, v_ref.shape[2]), 0)
        v_ref[h, head_width:, :] = jnp.where(at_row == 0, 1.0, 0.0).astype(jnp.bfloat16)

    def padded(part):
        return jnp.concatenate([part, jnp.zeros((rows, 128 - head_width), jnp.float32)], axis=1)

    def project(u):
        out = jnp.dot(held[u], weights[...], preferred_element_type=jnp.float32)
        seg = seg_at(starts, mine * blocks * chunks * rows + u * rows + row)
        same = lane - head_width == seg
        at = pl.ds(pl.multiple_of(u * rows, rows), rows)
        for h in range(heads):
            o = 3 * head_width * h
            q = padded(out[:, o:o + head_width] * scale)
            k = padded(out[:, o + head_width:o + 2 * head_width])
            v = out[:, o + 2 * head_width:o + 3 * head_width]
            q = jnp.where(lane < head_width, q, jnp.where(same, big_negative, 0.0))
            k = jnp.where(lane < head_width, k, jnp.where(same, 0.0, 1.0))
            q_ref[h, at, :] = q.astype(jnp.bfloat16)
            k_ref[h, at, :] = k.astype(jnp.bfloat16)
            v_ref[h, :head_width, at] = v.T.astype(jnp.bfloat16)

    inner = step - side == reach - 1

    def unit(j, i, parity):
        swap = jnp.logical_and(inner, step % 2 != parity)
        n = jnp.where(swap, reach - 1 - j % reach, j // chunks)
        c = jnp.where(swap, j // reach, j % chunks)
        n = n + side * (reach - 1 - 2 * n)
        return ((2 * n + parity) * np_ + (share + i) % np_) * chunks + c

    lifts = reach == 2 and np_ > 1
    inner_step, outer_step = reach - 1 + side, side * (steps - 1)

    def lifted(u, at_inner):
        return jnp.logical_and(at_inner, u // (chunks * np_) == outer_step)

    def lift(j, i, k):
        u = unit(j, i, core)
        here = piece(held, u, k)
        return remote(
            here, here, z_sem.at[(j * (np_ - 1) + i - 1) * parts_of_chunk + k],
            r_sem.at[u * parts_of_chunk + k],
            (side * reach + (step - side * reach + 1) % reach) * np_ + share, g,
        )

    def crosses(j):
        if lifts:
            return jnp.logical_not(lifted(unit(j, 0, core), inner))
        return j >= 0

    def climbs(j, i):
        return lifted(unit(j, i, core), jnp.logical_not(inner))

    early = jnp.logical_and(step == outer_step, step % 2 == core)

    def came(u, k):
        here = piece(held, u, k)
        return remote(here, here, p_sem.at[0], r_sem.at[u * parts_of_chunk + k], b, partner)

    def pair(j, i, k):
        u = unit(j, i, core)
        here = piece(held, u, k)
        return remote(
            here, here, p_sem.at[(j * np_ + i) * parts_of_chunk + k],
            r_sem.at[u * parts_of_chunk + k], b, partner,
        )

    def across(j, i, k):
        u = unit(j, 0, core)
        here = piece(held, u, k)
        return remote(
            here, here, y_sem.at[(j * (np_ - 1) + i - 1) * parts_of_chunk + k],
            r_sem.at[u * parts_of_chunk + k], b - share + (share + i) % np_, g,
        )

    def over(j, i, k):
        u = unit(j, 0, core)
        here = piece(held, u, k)
        other = side * reach + (step - side * reach + i) % reach
        return remote(
            here, here, x_sem.at[(j * (reach - 1) + i - 1) * parts_of_chunk + k],
            r_sem.at[u * parts_of_chunk + k], other * np_ + share, g,
        )

    count = reach * chunks

    def enters(j):
        return entry(unit(j, 0, core) // (chunks * np_), side) == step

    def take(j):
        u = unit(j, 0, core)
        for k in range(parts_of_chunk):
            @pl.when(jnp.logical_not(jnp.logical_and(u // chunks == b, home)))
            def _():
                came(u, k).wait_recv()

            @pl.when(enters(j))
            def _():
                for i in range(1, reach):
                    over(j, i, k).start()

            @pl.when(crosses(j))
            def _():
                for i in range(1, np_):
                    across(j, i, k).start()

            pair(j, 0, k).start()

    def arrive(u):
        for k in range(parts_of_chunk):
            came(u, k).wait_recv()

    def pass_on(j):
        for i in range(1, np_):
            for k in range(parts_of_chunk):
                came(unit(j, i, core), k).wait_recv()
                if lifts:
                    @pl.when(climbs(j, i))
                    def _():
                        lift(j, i, k).start()

                pair(j, i, k).start()

    with jax.named_scope("first"):
        take(0)
        take(1)
        pass_on(0)

        @pl.when(early)
        def _():
            pass_on(1)

        if count > 2:
            take(2)

    with jax.named_scope("weights"):
        @pl.when(own_slab)
        def _():
            load_own.wait()

        @pl.when(jnp.logical_not(own_slab))
        def _():
            give(0)[1].wait_recv()

    def gather(j, carry):
        project(unit(j, 0, core))

        @pl.when(j + 3 < count)
        def _():
            take(j + 3)

        @pl.when(jnp.logical_or(j >= 2, jnp.logical_and(j == 1, jnp.logical_not(early))))
        def _():
            pass_on(j)

        u = unit(j, 0, 1 - core)
        arrive(u)
        project(u)
        for i in range(1, np_):
            project(unit(j, i, core))
        for i in range(1, np_):
            u = unit(j, i, 1 - core)
            arrive(u)
            project(u)
        return carry

    with jax.named_scope("gather"):
        lax.fori_loop(0, count, gather, 0)

    def send(s):
        return remote(
            mixed_heads.at[s], parts.at[slot], s_sem.at[s], a_sem.at[slot], s, mine
        )

    tile = min(1024, blocks * block)
    tiles = blocks * block // tile

    def order(i):
        far = jnp.logical_or(i == 0, jnp.logical_and(i % 2 == 1, i < blocks - 1))
        away = (i + 1) // 2
        close = jnp.where(i == blocks - 1, blocks // 2 - 1, i // 2 - 1)
        out_step = side * (away // np_) + (1 - side) * (steps - 1 - away // np_)
        in_step = side * reach + (step - side * reach + 1 + close // np_) % reach
        n = jnp.where(far, out_step, in_step)
        m = jnp.where(far, away, close)
        return n * np_ + (share + 1 + m) % np_

    def score(i, h, n, top):
        at = pl.ds(pl.multiple_of(order(i) * block, block), block)
        keys = slice(n * tile, (n + 1) * tile)
        raw = lax.dot_general(
            k_ref[h, keys, :], q_ref[h, at, :], (((1,), (1,)), ((), ())),
            preferred_element_type=jnp.float32,
        )
        scores[h, keys, :] = raw
        return jnp.maximum(top, jnp.max(raw.reshape(tile // 8, 8, block), axis=0))

    def mix(h, n, top, total):
        keys = slice(n * tile, (n + 1) * tile)
        probs = jnp.exp2(scores[h, keys, :] - top).astype(jnp.bfloat16)
        return total + jnp.dot(v_ref[h, :, keys], probs, preferred_element_type=jnp.float32)

    lowest = jnp.full((8, block), -jnp.inf, jnp.float32)

    def attend_for(i, top):
        outs = []
        for h in range(heads):
            top = jnp.max(top, axis=0, keepdims=True)
            later = lowest
            total = jnp.zeros((v_ref.shape[1], block), jnp.float32)
            next_i, next_h = (i, h + 1) if h + 1 < heads else (jnp.minimum(i + 1, blocks - 1), 0)
            if heads == 1:
                for n in range(tiles):
                    total = mix(h, n, top, total)
                for n in range(tiles):
                    later = score(next_i, next_h, n, later)
            else:
                for n in range(tiles):
                    later = score(next_i, next_h, n, later)
                    total = mix(h, n, top, total)
            outs.append(total[:head_width] / total[head_width:head_width + 1])
            top = later
        s = order(i)
        mixed_heads[s] = jnp.concatenate(outs, axis=0).T.astype(jnp.bfloat16)
        kept = jnp.logical_and(home, s == b)

        @pl.when(jnp.logical_not(kept))
        def _():
            send(s).start()

        @pl.when(kept)
        def _():
            parts[slot] = mixed_heads[s]

        return top

    with jax.named_scope("attend"):
        top = lowest
        for n in range(tiles):
            top = score(0, 0, n, top)
        lax.fori_loop(0, blocks, attend_for, top)

    row = position * block + lax.broadcasted_iota(jnp.int32, (block, 128), 0)
    low = jnp.zeros((block, 128), jnp.int32)
    high = jnp.full((block, 128), blocks * groups * block, jnp.int32)
    for start in starts:
        low = jnp.where(row >= start, jnp.maximum(low, start), low)
        high = jnp.where(row < start, jnp.minimum(high, start), high)
    for t in range(taps):
        at = row + (t - half)
        masks[t] = jnp.where(jnp.logical_and(at >= low, at < high), 1.0, 0.0)

    part_width = parts.shape[2]
    together = max(1, 256 // part_width)
    with jax.named_scope("parts_wait"):
        loads[0].wait()
        total = frames_ref[...].astype(jnp.float32)
        for first in range(0, blocks, together):
            for i in range(first, first + together):
                @pl.when(jnp.logical_not(jnp.logical_and(home, slot == i)))
                def _():
                    remote(parts.at[i], parts.at[i], s_sem.at[i], a_sem.at[i], b, g).wait_recv()

            attended = jnp.concatenate([parts[first + i] for i in range(together)], axis=1)
            at = slice(first * part_width, (first + together) * part_width)
            total = total + jnp.dot(attended, w_out[at, :], preferred_element_type=jnp.float32)
            if first + together < blocks:
                mixed[...] = total
                total = mixed[...]

    with jax.named_scope("mid_mm"):
        residual[...] = total.astype(jnp.bfloat16)
        conv_in = normalize(residual[...].astype(jnp.float32), conv_gain_ref[...]).astype(jnp.bfloat16)
        loads[1].wait()
        span = 256
        for n in range(0, width, span):
            a = jnp.dot(conv_in, w_glu[:, n:n + span], preferred_element_type=jnp.float32)
            gate = jnp.dot(
                conv_in, w_glu[:, width + n:width + n + span], preferred_element_type=jnp.float32
            )
            gated = (a * jax.nn.sigmoid(gate)).astype(jnp.bfloat16)
            edge[0, :, n:n + span] = gated[:rim]
            edge[1, :, n:n + span] = gated[block - rim:]
            for c in range(0, span, 128):
                extended[(n + c) // 128, rim:rim + block, :] = gated[:, c:c + 128].astype(jnp.float32)

    to_next = remote(
        edge.at[1], halo.at[0], hs_sem.at[1], hr_sem.at[0], after % blocks, after // blocks
    )
    to_prev = remote(
        edge.at[0], halo.at[1], hs_sem.at[0], hr_sem.at[1], before % blocks, before // blocks
    )

    @pl.when(has_after)
    def _():
        to_next.start()

    @pl.when(has_before)
    def _():
        to_prev.start()

    spans = -(-taps // 8)

    def convolve(strips):
        def column(c, carry):
            cols = pl.ds(pl.multiple_of(c * 128, 128), 128)
            for r, strip in strips:
                acc = jnp.zeros((strip, 128), jnp.float32)
                for p in range(8):
                    o = rim + r + p - half
                    slab = extended[c, o:o + strip + 8 * (spans - 1), :]
                    for t in range(p, taps, 8):
                        x = slab[t - p:t - p + strip] * masks[t, r:r + strip, :]
                        acc = acc + x * depth_ref[t:t + 1, cols]
                mixed[r:r + strip, cols] = acc
            return carry

        lax.fori_loop(0, width // 128, column, 0)

    with jax.named_scope("conv_mid"):
        convolve([(r, min(64, block - rim - r)) for r in range(rim, block - rim, 64)])
    with jax.named_scope("tail_mm"):
        loads[2].wait()
        out_ref[0, rim:block - rim] = finished(
            mixed[rim:block - rim], residual[rim:block - rim], depth_gain_ref[...], w_proj[...]
        )
    with jax.named_scope("halo_wait"):
        for i, present in ((0, has_before), (1, has_after)):
            @pl.when(present)
            def _():
                remote(
                    edge.at[i], halo.at[i], hs_sem.at[i], hr_sem.at[i], b, g
                ).wait_recv()

            @pl.when(jnp.logical_not(present))
            def _():
                halo[i] = jnp.zeros(halo.shape[1:], jnp.bfloat16)

    with jax.named_scope("conv_edge"):
        for c in range(width // 128):
            at = slice(128 * c, 128 * c + 128)
            extended[c, :rim, :] = halo[0, :, at].astype(jnp.float32)
            extended[c, rim + block:2 * rim + block, :] = halo[1, :, at].astype(jnp.float32)
        convolve([(0, rim), (block - rim, rim)])
    with jax.named_scope("tail_edge"):
        ends = finished(
            jnp.concatenate([mixed[:rim], mixed[block - rim:]], axis=0),
            jnp.concatenate([residual[:rim], residual[block - rim:]], axis=0),
            depth_gain_ref[...], w_proj[...],
        )
        out_ref[0, :rim] = ends[:rim]
        out_ref[0, block - rim:] = ends[rim:]

    with jax.named_scope("drain"):
        for c in range(chunks):
            for k in range(parts_of_chunk):
                @pl.when(jnp.logical_not(self_kept))
                def _():
                    direct(c, k).wait_send()

        for other in range(groups):
            source, copy = give(other)

            @pl.when(jnp.logical_and(source == g, other != g))
            def _():
                copy.wait_send()

        def drain(j, carry):
            for k in range(parts_of_chunk):
                @pl.when(enters(j))
                def _():
                    for i in range(1, reach):
                        over(j, i, k).wait_send()

                @pl.when(crosses(j))
                def _():
                    for i in range(1, np_):
                        across(j, i, k).wait_send()

                if lifts:
                    for i in range(1, np_):
                        @pl.when(climbs(j, i))
                        def _():
                            lift(j, i, k).wait_send()

                for i in range(np_):
                    pair(j, i, k).wait_send()
            return carry

        lax.fori_loop(0, count, drain, 0)

        for i in range(blocks):
            @pl.when(jnp.logical_not(jnp.logical_and(home, b == i)))
            def _():
                send(i).wait_send()

        @pl.when(has_after)
        def _():
            to_next.wait_send()

        @pl.when(has_before)
        def _():
            to_prev.wait_send()


def body(
    frames, utt_lengths, attn_gain, w_qkv, w_out, conv_gain, w_glu, w_depth, depth_gain, w_proj
):
    rows, width = frames.shape[1:]
    blocks, groups = lax.axis_size("blk"), lax.axis_size("grp")
    head_width = width // HEADS
    np_ = blocks // groups
    columns = w_qkv.shape[1] // np_
    heads = columns // (3 * head_width)
    window = rows * blocks
    chunks = 2 if rows % 32 == 0 else 1
    parts_of_chunk = 2 if rows // chunks % 32 == 0 else 1
    reach = blocks // np_ // 2
    taps = w_depth.shape[0]
    rim = -(-(taps // 2) // 16) * 16
    vm = pl.BlockSpec(memory_space=pltpu.VMEM)
    hbm = pl.BlockSpec(memory_space=pl.ANY)
    return pl.pallas_call(
        functools.partial(block_kernel, blocks, groups, parts_of_chunk, head_width),
        out_shape=jax.ShapeDtypeStruct((1, rows, width), jnp.bfloat16),
        in_specs=[hbm] * 10,
        out_specs=vm,
        scratch_shapes=[
            pltpu.SMEM(utt_lengths.shape, jnp.int32),
            pltpu.VMEM((rows, width), jnp.bfloat16),
            pltpu.VMEM((1, width), jnp.float32),
            pltpu.VMEM((1, width), jnp.float32),
            pltpu.VMEM(w_depth.shape, jnp.float32),
            pltpu.VMEM((1, width), jnp.float32),
            pltpu.VMEM((chunks, rows // chunks, width), jnp.bfloat16),
            pltpu.VMEM((blocks * chunks, rows // chunks, width), jnp.bfloat16),
            pltpu.VMEM((width, columns), jnp.bfloat16),
            pltpu.VMEM((width, columns), jnp.bfloat16),
            pltpu.VMEM((heads, window, 128), jnp.bfloat16),
            pltpu.VMEM((heads, window, 128), jnp.bfloat16),
            pltpu.VMEM((heads, head_width + 16, window), jnp.bfloat16),
            pltpu.VMEM((heads, window, rows), jnp.float32),
            pltpu.VMEM((blocks, rows, heads * head_width), jnp.bfloat16),
            pltpu.VMEM((blocks, rows, heads * head_width), jnp.bfloat16),
            pltpu.VMEM(w_out.shape, jnp.bfloat16),
            pltpu.VMEM(w_glu.shape, jnp.bfloat16),
            pltpu.VMEM(w_proj.shape, jnp.bfloat16),
            pltpu.VMEM((taps, rows, 128), jnp.float32),
            pltpu.VMEM((rows, width), jnp.bfloat16),
            pltpu.VMEM((2, rim, width), jnp.bfloat16),
            pltpu.VMEM((2, rim, width), jnp.bfloat16),
            pltpu.VMEM((width // 128, rows + 2 * rim + 8, 128), jnp.float32),
            pltpu.VMEM((rows, width), jnp.float32),
            pltpu.SemaphoreType.DMA((5,)),
            pltpu.SemaphoreType.DMA((6,)),
            pltpu.SemaphoreType.DMA((groups,)),
            pltpu.SemaphoreType.DMA((1,)),
            pltpu.SemaphoreType.DMA((chunks * parts_of_chunk,)),
            pltpu.SemaphoreType.DMA((reach * chunks * (reach - 1) * parts_of_chunk,)),
            pltpu.SemaphoreType.DMA((reach * chunks * max(np_ - 1, 1) * parts_of_chunk,)),
            pltpu.SemaphoreType.DMA((reach * chunks * max(np_ - 1, 1) * parts_of_chunk,)),
            pltpu.SemaphoreType.DMA((reach * chunks * np_ * parts_of_chunk,)),
            pltpu.SemaphoreType.DMA((blocks * chunks * parts_of_chunk,)),
            pltpu.SemaphoreType.DMA((blocks,)),
            pltpu.SemaphoreType.DMA((blocks,)),
            pltpu.SemaphoreType.DMA((2,)),
            pltpu.SemaphoreType.DMA((2,)),
        ],
        compiler_params=pltpu.CompilerParams(
            collective_id=0, has_side_effects=True, vmem_limit_bytes=VMEM_LIMIT),
        name="block",
    )(
        utt_lengths, frames[0], attn_gain[None], conv_gain[None], w_depth, depth_gain[None],
        w_qkv, w_out, w_glu, w_proj,
    )


def solution(mesh):
    in_specs = (P("grp", "blk", None), P(), P(), P(None, "grp"), P(), P(), P(), P(), P(), P())
    out_specs = P("grp", "blk", None)
    return jax.shard_map(body, mesh=mesh, in_specs=in_specs, out_specs=out_specs, check_vma=False)
```
